256 devices in a mesh: rep: 2 (over y), gx: 128 (over x, z, core).
Axes of the slice: x: 4, y: 2, z: 16, core: 2. Of those that a mesh axis runs over, the one named last changes fastest.
The devices are a block of a 4x16x16 slice.
Arguments:
- positions: float32 [3, 262144], P(None, ('rep', 'gx')), parts along dimension 1, may hold values from 0 to 8, as said below
- field: float32 [3, 262144], P(None, ('rep', 'gx')), parts along dimension 1, may hold values from -45 to 45
- inv_polar: float32 [262144], P(('rep', 'gx')), parts along dimension 0, may hold values from 2 to 8
- x_spline: float32 [2, 5, 262144], P(None, None, ('rep', 'gx')), parts along dimension 2, may hold values from -1 to 1, as said below
- yz_spline: float32 [4, 262144, 128], P(None, ('rep', 'gx')), parts along dimension 1, may hold values from -1 to 1, as said below
- tile_list: int32 [2048, 7], P(('rep', 'gx')), parts along dimension 0, may hold values from 0 to 13, as said below
- tile_count: int32 [2048], P(('rep', 'gx')), parts along dimension 0, may hold values from 1 to 7, as said below
Outputs:
- dipoles: float32 [3, 262144], P(None, ('rep', 'gx')), parts along dimension 1
- residual: float32 [3, 262144], P(None, ('rep', 'gx')), parts along dimension 1
The draws below stay inside these ranges and needn't reach their ends.
There are 2 independent parts, one for each index of `rep`. The reference program is written for one: setup_inputs(seed, part) draws one part's arguments, and reference() takes and returns one part's arrays. A program takes and returns all parts, laid end to end along the dimension named above; each array names one. Nothing has to cross between parts.
Inputs may be any that keep to these rules, and one draw needn't show every extreme that they name: `positions`: the first coordinate of an atom of block b of its slab lies in [b, b + 1); the other two lie in [0, 2). x_spline[0, k, i] and x_spline[1, k, i] are the cardinal B-spline of order 5 and its derivative at u_i + 4 - k for some u_i in [0, 1). `yz_spline`: rows 0 and 1 hold, for each atom, the cardinal B-spline of order 5 and its derivative at u + 4 - k placed at grid line (t + k) mod 128 for k < 5, for some start t and some u in [0, 1), and zero elsewhere; rows 2 and 3 likewise with their own start and offset. `tile_list`: row g = s * 8 + b lists in rising order the extended blocks b + 3 + e, -3 <= e <= 3, for which global blocks g and g + e (modulo 1024) are neighbours; being neighbours is symmetric and always holds for e = 0; entries from tile_count[g] on equal b + 3. `tile_count`: global block 0 has all 7 neighbours.
All inputs are finite; a program needn't handle non-finite values.
Results may differ from the reference program's by a relative error of at most 0.0003.
Values sent between devices are 32-bit elements; how exact they have to be, the bound alone decides.
A program may use at most 64 MiB of HBM per device.

```python
import math
import jax
import jax.numpy as jnp
from jax import lax

GRID = 128
ORDER = 5
TILE = 128
HALO_BLK = 3
ITERS = 3
ATOM_DEV = 1024
NNB = 7
ATOMS = 131072
SLAB_BLOCKS = 8
BLOCKS = 1024
N_GX = 128


def cardinal(order_now, at_point):
    if order_now == 2:
        return jnp.maximum(0.0, 1.0 - jnp.abs(at_point - 1.0))
    lower_part = cardinal(order_now - 1, at_point)
    upper_part = cardinal(order_now - 1, at_point - 1.0)
    return (at_point * lower_part + (order_now - at_point) * upper_part) / (order_now - 1)


def spline_pair(frac):
    shifts = (ORDER - 1 - jnp.arange(ORDER, dtype=jnp.int32)).astype(jnp.float32)
    points = frac[None, :] + shifts[:, None]
    spline_value = cardinal(ORDER, points)
    spline_slope = cardinal(ORDER - 1, points) - cardinal(ORDER - 1, points - 1.0)
    return (spline_value, spline_slope)


def draw_positions(key, part):
    atom_index = jnp.arange(ATOMS, dtype=jnp.int32)
    block_of = (atom_index % ATOM_DEV // TILE).astype(jnp.float32)
    uniform_draw = jax.random.uniform(key, (3, ATOMS), jnp.float32)
    return jnp.stack([block_of + uniform_draw[0], 2.0 * uniform_draw[1], 2.0 * uniform_draw[2]]).astype(jnp.float32)


def draw_field(key, part):
    atom_index = jnp.arange(ATOMS, dtype=jnp.int32)
    slab_of = (atom_index // ATOM_DEV).astype(jnp.float32)
    slab_total = ATOMS // ATOM_DEV
    ramp = 1.0 + 2.0 * slab_of / max(slab_total - 1, 1)
    normal_draw = jnp.clip(jax.random.normal(jax.random.fold_in(key, 1), (3, ATOMS), jnp.float32), -4.0, 4.0)
    return (normal_draw * ramp[None, :]).astype(jnp.float32)


def draw_x_spline(key, part):
    frac = jax.random.uniform(key, (ATOMS,), jnp.float32)
    spline_value, spline_slope = spline_pair(frac)
    return jnp.stack([spline_value, spline_slope]).astype(jnp.float32)


def draw_yz_spline(key, part):
    grid_lines = jnp.arange(GRID, dtype=jnp.int32)
    tables = []
    for axis_code in (1, 2):
        sub_key = jax.random.fold_in(key, axis_code)
        start_line = jax.random.randint(jax.random.fold_in(sub_key, 1), (ATOMS,), 0, GRID, dtype=jnp.int32)
        frac = jax.random.uniform(jax.random.fold_in(sub_key, 2), (ATOMS,), jnp.float32)
        spline_value, spline_slope = spline_pair(frac)
        dense_value = jnp.zeros((ATOMS, GRID), jnp.float32)
        dense_slope = jnp.zeros((ATOMS, GRID), jnp.float32)
        for spline_step in range(ORDER):
            matches = ((start_line + spline_step) % GRID)[:, None] == grid_lines[None, :]
            dense_value = dense_value + jnp.where(matches, spline_value[spline_step][:, None], 0.0)
            dense_slope = dense_slope + jnp.where(matches, spline_slope[spline_step][:, None], 0.0)
        tables.append(dense_value)
        tables.append(dense_slope)
    return jnp.stack(tables).astype(jnp.float32)


def neighbour_table(key):
    block_ids = jnp.arange(BLOCKS, dtype=jnp.int32)
    reach = jnp.arange(1, HALO_BLK + 1, dtype=jnp.int32)
    coins = jax.random.randint(jax.random.fold_in(key, 7), (BLOCKS, HALO_BLK), 0, 2, dtype=jnp.int32)
    first_block = block_ids == 0
    partner = (block_ids[:, None] + reach[None, :]) % BLOCKS
    coins = jnp.where(first_block[:, None] | first_block[partner], 1, coins)
    upper_side = coins
    lower_rows = (block_ids[:, None] - reach[None, :]) % BLOCKS
    lower_side = coins[lower_rows, (reach - 1)[None, :]]
    linked = jnp.concatenate([lower_side[:, ::-1], jnp.ones((BLOCKS, 1), jnp.int32), upper_side], axis=1)
    live_count = jnp.sum(linked, axis=1).astype(jnp.int32)
    slot_ids = jnp.arange(NNB, dtype=jnp.int32)
    sort_keys = jnp.where(linked == 1, slot_ids[None, :], NNB + slot_ids[None, :])
    ordering = jnp.argsort(sort_keys, axis=1, stable=True).astype(jnp.int32)
    local_block = (block_ids % SLAB_BLOCKS)[:, None]
    entries = jnp.where(slot_ids[None, :] < live_count[:, None], local_block + ordering, local_block + HALO_BLK)
    return (entries.astype(jnp.int32), live_count)


def draw_tile_list(key, part):
    entries, live_count = neighbour_table(key)
    return entries


def draw_tile_count(key, part):
    entries, live_count = neighbour_table(key)
    return live_count.astype(jnp.int32)


def levels(stream_key, shape, split, low, high):
    gain, own = 1.0, jax.random.fold_in(stream_key, 6)
    for dim, shards_of in split:
        draws = jnp.exp(jax.random.uniform(jax.random.fold_in(own, dim), (shards_of,), jnp.float32, low / len(split), high / len(split)))
        gain = gain * jnp.repeat(draws, shape[dim] // shards_of).reshape([-1 if axis == dim else 1 for axis in range(len(shape))])
    return gain


def setup_inputs(seed: int = 0, part: int = 0) -> dict:
    keys = jax.random.split(jax.random.key(seed), 8)
    part_keys = jax.random.split(jax.random.fold_in(keys[7], part), 8)
    positions = draw_positions(jax.random.fold_in(jax.random.fold_in(keys[7], part), 71), part)
    field = draw_field(jax.random.fold_in(jax.random.fold_in(keys[7], part), 71), part)
    inv_polar = jnp.clip(jnp.exp(math.log(8.0) - 1.3862944 * jax.random.uniform(part_keys[2], (ATOMS,), jnp.float32) ** levels(part_keys[2], (ATOMS,), ((0, 128),), -0.2, 0.2)), 2.0, 8.0)
    x_spline = draw_x_spline(jax.random.fold_in(jax.random.fold_in(keys[7], part), 71), part)
    yz_spline = draw_yz_spline(jax.random.fold_in(jax.random.fold_in(keys[7], part), 71), part)
    tile_list = draw_tile_list(jax.random.fold_in(jax.random.fold_in(keys[7], part), 71), part)
    tile_count = draw_tile_count(jax.random.fold_in(jax.random.fold_in(keys[7], part), 71), part)
    return {"positions": positions, "field": field, "inv_polar": inv_polar, "x_spline": x_spline, "yz_spline": yz_spline, "tile_list": tile_list, "tile_count": tile_count}


PAIR_C = 0.025
RECIP_C = 8192.0
DAMP = 0.0008
EXACT = lax.Precision.HIGHEST

def pair_field(home_pos, ext_pos, ext_vec, tile_rows, live_counts):
    slab_blocks = home_pos.shape[1] // TILE
    ext_blocks = ext_pos.shape[1] // TILE
    home_blocks = home_pos.reshape(3, slab_blocks, TILE).transpose(1, 0, 2)
    pos_blocks = ext_pos.reshape(3, ext_blocks, TILE)
    vec_blocks = ext_vec.reshape(3, ext_blocks, TILE)
    slot_index = jnp.arange(tile_rows.shape[1], dtype=jnp.int32)
    self_pair = jnp.eye(TILE, dtype=bool)

    def one_block(carried, scan_item):
        home_block, tile_row, live_count, block_index = scan_item
        near_pos = jnp.take(pos_blocks, tile_row, axis=1)
        near_vec = jnp.take(vec_blocks, tile_row, axis=1)
        offsets = home_block[:, None, :, None] - near_pos[:, :, None, :]
        distance_sq = lax.optimization_barrier(jnp.sum(offsets * offsets, axis=0)) + 1.0
        inverse = lax.rsqrt(distance_sq)
        third_power = inverse * inverse * inverse
        fifth_power = third_power * inverse * inverse
        same_block = (tile_row == block_index + HALO_BLK)[:, None, None]
        live_mask = (slot_index < live_count)[:, None, None] & ~(same_block & self_pair[None])
        third_power = jnp.where(live_mask, third_power, 0.0)
        fifth_power = jnp.where(live_mask, fifth_power, 0.0)
        projection = lax.optimization_barrier(jnp.sum(offsets * near_vec[:, :, None, :], axis=0))
        field_sum = lax.optimization_barrier(jnp.sum(third_power[None] * near_vec[:, :, None, :] - 3.0 * (fifth_power * projection)[None] * offsets, axis=(1, 3)))
        return (carried, PAIR_C * field_sum)
    block_ids = jnp.arange(slab_blocks, dtype=jnp.int32)
    unused_carry, blocks_out = lax.scan(one_block, jnp.zeros((), jnp.float32), (home_blocks, tile_rows, live_counts, block_ids))
    return blocks_out.transpose(1, 0, 2).reshape(3, slab_blocks * TILE)

def slab_weights(local_plane, x_spline, planes):
    spline_steps = jnp.arange(ORDER, dtype=jnp.int32)
    plane_index = jnp.arange(planes, dtype=jnp.int32)
    matches = local_plane[None, :, None] + spline_steps[:, None, None] == plane_index[None, None, :]
    spline_value = lax.optimization_barrier(jnp.sum(jnp.where(matches, x_spline[0][:, :, None], 0.0), axis=0))
    spline_slope = lax.optimization_barrier(jnp.sum(jnp.where(matches, x_spline[1][:, :, None], 0.0), axis=0))
    return (spline_value, spline_slope)

def spread_dipoles(vector, spline_value, spline_slope, yz_spline):
    atoms_here = spline_value.shape[0]
    planes = spline_value.shape[1]
    grid_lines = yz_spline.shape[2]
    lead_terms = (vector[0][:, None] * spline_slope)[:, :, None] * yz_spline[0][:, None, :]
    lead_terms = lead_terms + (vector[1][:, None] * spline_value)[:, :, None] * yz_spline[1][:, None, :]
    tail_terms = (vector[2][:, None] * spline_value)[:, :, None] * yz_spline[0][:, None, :]
    contract = (((0,), (0,)), ((), ()))
    charge = lax.dot_general(lead_terms.reshape(atoms_here, planes * grid_lines), yz_spline[2], contract, precision=EXACT)
    charge = charge + lax.dot_general(tail_terms.reshape(atoms_here, planes * grid_lines), yz_spline[3], contract, precision=EXACT)
    return charge.reshape(planes, grid_lines, grid_lines)

def gather_field(potential, spline_value, spline_slope, yz_spline):
    planes = potential.shape[0]
    grid_lines = potential.shape[1]
    atoms_here = spline_value.shape[0]
    flat_grid = potential.reshape(planes * grid_lines, grid_lines)
    contract = (((1,), (1,)), ((), ()))
    plain_sum = lax.dot_general(yz_spline[2], flat_grid, contract, precision=EXACT).reshape(atoms_here, planes, grid_lines)
    tilted_sum = lax.dot_general(yz_spline[3], flat_grid, contract, precision=EXACT).reshape(atoms_here, planes, grid_lines)
    first_comp = lax.optimization_barrier(jnp.sum(spline_slope[:, :, None] * yz_spline[0][:, None, :] * plain_sum, axis=(1, 2)))
    second_comp = lax.optimization_barrier(jnp.sum(spline_value[:, :, None] * yz_spline[1][:, None, :] * plain_sum, axis=(1, 2)))
    third_comp = lax.optimization_barrier(jnp.sum(spline_value[:, :, None] * yz_spline[0][:, None, :] * tilted_sum, axis=(1, 2)))
    return jnp.stack([first_comp, second_comp, third_comp])

def reference_kernel():
    freq = jnp.arange(GRID, dtype=jnp.int32)
    signed = jnp.where(freq <= GRID // 2, freq, freq - GRID).astype(jnp.float32)
    last_freq = jnp.arange(GRID // 2 + 1, dtype=jnp.int32).astype(jnp.float32)
    mode_sq = signed[:, None, None] * signed[:, None, None] + signed[None, :, None] * signed[None, :, None] + last_freq[None, None, :] * last_freq[None, None, :]
    safe_sq = jnp.where(mode_sq > 0, mode_sq, 1.0)
    return jnp.where(mode_sq > 0, RECIP_C * jnp.exp(-DAMP * safe_sq) / safe_sq, 0.0)

def reference(positions, field, inv_polar, x_spline, yz_spline, tile_list, tile_count):
    slabs = N_GX
    planes = GRID // slabs
    extent = planes + 4
    halo_atoms = HALO_BLK * TILE
    slab_blocks = ATOM_DEV // TILE
    slab_ids = jnp.arange(slabs, dtype=jnp.int32)
    shift_x = jnp.concatenate([jnp.full((halo_atoms,), -1.0 * slab_blocks, jnp.float32), jnp.zeros((ATOM_DEV,), jnp.float32), jnp.full((halo_atoms,), 1.0 * slab_blocks, jnp.float32)])
    kernel = reference_kernel()
    place = slab_ids[:, None] * planes + jnp.arange(extent, dtype=jnp.int32)[None, :]
    local_plane = (jnp.arange(ATOM_DEV, dtype=jnp.int32) * planes // ATOM_DEV).astype(jnp.int32)

    def wrap_pad(array):
        return jnp.concatenate([array[:, -halo_atoms:], array, array[:, :halo_atoms]], axis=1)
    pos_pad = wrap_pad(positions)

    def slab_parts(slab):
        begin = slab * ATOM_DEV
        own_pos = lax.dynamic_slice_in_dim(positions, begin, ATOM_DEV, 1)
        ext_pos = lax.dynamic_slice_in_dim(pos_pad, begin, ATOM_DEV + 2 * halo_atoms, 1)
        ext_pos = ext_pos.at[0].add(shift_x)
        splines = lax.dynamic_slice_in_dim(x_spline, begin, ATOM_DEV, 2)
        dense = lax.dynamic_slice_in_dim(yz_spline, begin, ATOM_DEV, 1)
        tile_rows = lax.dynamic_slice_in_dim(tile_list, slab * slab_blocks, slab_blocks, 0)
        live_counts = lax.dynamic_slice_in_dim(tile_count, slab * slab_blocks, slab_blocks, 0)
        spline_value, spline_slope = slab_weights(local_plane, splines, extent)
        return (own_pos, ext_pos, spline_value, spline_slope, dense, tile_rows, live_counts)

    def apply(vector):
        vec_pad = wrap_pad(vector)

        def near_and_charge(slab):
            parts = slab_parts(slab)
            begin = slab * ATOM_DEV
            ext_vec = lax.dynamic_slice_in_dim(vec_pad, begin, ATOM_DEV + 2 * halo_atoms, 1)
            own_vec = lax.dynamic_slice_in_dim(vector, begin, ATOM_DEV, 1)
            near_field = pair_field(parts[0], parts[1], ext_vec, parts[5], parts[6])
            charge = spread_dipoles(own_vec, parts[2], parts[3], parts[4])
            return (near_field, charge)
        near_all, charges = lax.map(near_and_charge, slab_ids)
        padded = jnp.zeros((GRID + 4, GRID, GRID), jnp.float32).at[place].add(charges)
        whole = padded[2:GRID + 2]
        whole = whole.at[GRID - 2:].add(padded[:2]).at[:2].add(padded[GRID + 2:])
        potential = jnp.fft.irfftn(jnp.fft.rfftn(whole) * kernel, s=whole.shape)
        pot_pad = jnp.concatenate([potential[GRID - 2:], potential, potential[:2]], axis=0)

        def far_part(scan_item):
            slab, local_pot = scan_item
            parts = slab_parts(slab)
            return gather_field(local_pot, parts[2], parts[3], parts[4])
        far_all = lax.map(far_part, (slab_ids, pot_pad[place]))
        near_whole = near_all.transpose(1, 0, 2).reshape(3, ATOMS)
        far_whole = far_all.transpose(1, 0, 2).reshape(3, ATOMS)
        return inv_polar[None, :] * vector + far_whole - near_whole
    dipoles = jnp.zeros_like(field)
    residual = field
    precond = field / inv_polar[None, :]
    direction = precond
    rz_now = jnp.sum(residual * precond)
    for sweep_index in range(ITERS):
        applied = apply(direction)
        step_size = rz_now / jnp.sum(direction * applied)
        dipoles = dipoles + step_size * direction
        residual = residual - step_size * applied
        if sweep_index + 1 < ITERS:
            precond = residual / inv_polar[None, :]
            rz_next = jnp.sum(residual * precond)
            direction = precond + rz_next / rz_now * direction
            rz_now = rz_next
    return (dipoles, residual)
```

```python
import functools

import jax
import jax.numpy as jnp
import numpy as np
from jax import lax
from jax.experimental import pallas as pl
from jax.experimental.pallas import tpu as pltpu
from jax.sharding import PartitionSpec as P

GRID = 128
ORDER = 5
TILE = 128
HALO_BLK = 3
ITERS = 3
PAIR_C = 0.025
RECIP_C = 8192.0
DAMP = 0.0008
EXACT = lax.Precision.HIGHEST
MESH = pl.DeviceIdType.MESH
F32 = jnp.float32
BF16 = jnp.bfloat16
NX = 4
NC = 2
OFFSETS = (-2, 2, -1, 1)


def far_first(count):
    return sorted(range(1, count), key=lambda d: -min(d, count - d))


def basis(size):
    freq = np.arange(size)
    half = size // 2
    mode = np.where(freq <= half, freq, freq - half)
    angle = (mode[:, None] * np.arange(size)[None, :] % size) * (2.0 * np.pi / size)
    return np.where((freq <= half)[:, None], np.cos(angle), np.sin(angle))


def split(x):
    hi = x.astype(BF16)
    return hi, (x - hi.astype(F32)).astype(BF16)


def exact_dot(a, b):
    return jnp.dot(a, b, precision=EXACT, preferred_element_type=F32)


def fast_dot(a, b):
    return jnp.dot(a, b, preferred_element_type=F32)


def mode_of(freq, size):
    half = size // 2
    mode = jnp.where(freq <= half, freq, freq - half)
    weight = jnp.where((freq == 0) | (freq == half), 1.0 / size, 2.0 / size)
    return mode.astype(F32), weight.astype(F32)


def solve_kernel(
    n,
    tile_list,
    tile_count,
    pos,
    field,
    inv_polar,
    x_spline,
    yz,
    four,
    four_t,
    four_x,
    four_xt,
    dip_out,
    res_out,
    link,
    ext,
    home,
    pair_acc,
    near,
    far,
    y_t,
    dy_t,
    zz,
    zt3,
    lhs_hi,
    lhs_lo,
    rim,
    rim_in,
    pot,
    pot_in,
    pot3,
    green,
    f1_src,
    f1_dst,
    f2_src,
    f2_dst,
    a_src,
    a_dst,
    b_src,
    b_dst,
    ra_src,
    ra_dst,
    rb_src,
    rb_dst,
    vecs,
    scal,
    v_ss,
    v_rs,
    c_ss,
    c_rs,
    h_ss,
    h_rs,
    f1_ss,
    f1_rs,
    f2_ss,
    f2_rs,
    a_ss,
    a_rs,
    b_ss,
    b_rs,
    ra_ss,
    ra_rs,
    rb_ss,
    rb_rs,
):
    nq = NX * NC
    nz = n // nq
    me = lax.axis_index("gx")
    my_q = (me // (nz * NC)) * NC + me % NC
    my_z = me % (nz * NC) // NC
    blocks = pos.shape[1] // TILE
    atoms = pos.shape[1]

    def at(q, z):
        return (q // NC) * (nz * NC) + z * NC + q % NC

    def q_peer(d):
        q = (my_q + d) % nq
        return q, at(q, my_z)

    def z_peer(d):
        z = (my_z + d) % nz
        return z, at(my_q, z)

    def to(d):
        return (me + d + n) % n

    def copy(src, dst, ss, rs, peer):
        return pltpu.make_async_remote_copy(
            src_ref=src, dst_ref=dst, send_sem=ss, recv_sem=rs,
            device_id={"gx": peer}, device_id_type=MESH,
        )

    def rows(i, size):
        return pl.ds(pl.multiple_of(i * size, size), size)

    barrier = pltpu.get_barrier_semaphore()
    for d in far_first(nz):
        pl.semaphore_signal(barrier, inc=1, device_id={"gx": z_peer(d)[1]}, device_id_type=MESH)
    for d in far_first(nq):
        pl.semaphore_signal(barrier, inc=1, device_id={"gx": q_peer(d)[1]}, device_id_type=MESH)
    for d in OFFSETS:
        pl.semaphore_signal(barrier, inc=1, device_id={"gx": to(d)}, device_id_type=MESH)

    def link_row(b, carry):
        for e in range(2 * HALO_BLK + 1):
            total = jnp.float32(0.0)
            for k in range(tile_list.shape[1]):
                hit = (tile_list[b, k] == b + e) & (k < tile_count[b])
                total = total + jnp.where(hit, jnp.float32(1.0), jnp.float32(0.0))
            link[b, e] = total
        return carry

    lax.fori_loop(0, blocks, link_row, 0)

    def prepare(b, carry):
        cols = rows(b, TILE)
        y_t[:, cols] = yz[0, cols, :].T
        dy_t[:, cols] = yz[1, cols, :].T
        for part in range(2):
            z_here = yz[2 + part, cols, :]
            hi, lo = split(z_here)
            at_rows = pl.ds(pl.multiple_of(part * atoms + b * TILE, TILE), TILE)
            zz[at_rows, :GRID] = hi
            zz[at_rows, GRID:] = lo
            hi_t, lo_t = split(z_here.T)
            zt3[:GRID, at_rows] = hi_t
            zt3[GRID : 2 * GRID, at_rows] = hi_t
            zt3[2 * GRID :, at_rows] = lo_t
        here = pos[:, cols]
        for c in range(3):
            home[c, cols, :] = jnp.broadcast_to(here[c : c + 1], (TILE, TILE)).T
        ext[HALO_BLK + b, 3:6, :] = here
        return carry

    lax.fori_loop(0, blocks, prepare, 0)

    row_freq = lax.broadcasted_iota(jnp.int32, (GRID, GRID), 0)
    col_freq = lax.broadcasted_iota(jnp.int32, (GRID, GRID), 1)
    kx, wx = mode_of(row_freq, GRID)
    kz, wz = mode_of(col_freq, GRID)
    ky, wy = mode_of(jnp.full((GRID, GRID), my_q * nz + my_z, jnp.int32), GRID)
    mode_sq = kx * kx + ky * ky + kz * kz
    safe_sq = jnp.where(mode_sq > 0, mode_sq, 1.0)
    green[...] = jnp.where(mode_sq > 0, RECIP_C * jnp.exp(-DAMP * safe_sq) / safe_sq, 0.0) * wx * wy * wz

    ip = inv_polar[...]
    R, U, W, PP, S, Q, Z, X, M = range(9)
    vecs[R] = field[...]
    vecs[U] = field[...] / ip
    vecs[M] = vecs[U]
    for name in (W, PP, S, Q, Z, X):
        vecs[name] = jnp.zeros_like(field)
    scal[...] = jnp.ones_like(scal)
    ra_src[...] = jnp.zeros_like(ra_src)
    pl.semaphore_wait(barrier, (nz - 1) + (nq - 1) + len(OFFSETS))

    def reduce_a():
        return [copy(ra_src, ra_dst.at[my_z], ra_ss.at[d], ra_rs.at[d], z_peer(d)[1]) for d in far_first(nz)]

    def reduce_b():
        return [copy(rb_src, rb_dst.at[my_q], rb_ss.at[d], rb_rs.at[d], q_peer(d)[1]) for d in far_first(nq)]

    def reduce_start():
        g = vecs[R] * vecs[U]
        h = vecs[W] * vecs[U]
        for row, value in ((0, g), (1, h)):
            folded = sum(value[:, k * TILE : (k + 1) * TILE] for k in range(atoms // TILE))
            ra_src[row : row + 1, :] = jnp.sum(folded, axis=0, keepdims=True)
        ra_dst[my_z] = ra_src[...]
        for c in reduce_a():
            c.start()

    def reduce_middle():
        for c in reduce_a():
            c.wait_recv()
        rb_src[...] = jnp.sum(ra_dst[...], axis=0)
        rb_dst[my_q] = rb_src[...]
        for c in reduce_b():
            c.start()

    def reduce_end():
        for c in reduce_b():
            c.wait_recv()
        sums = jnp.sum(jnp.sum(rb_dst[...], axis=0), axis=1, keepdims=True)
        for c in reduce_a():
            c.wait_send()
        for c in reduce_b():
            c.wait_send()
        scal[2] = jnp.broadcast_to(sums, (8, TILE))

    def vec_copies():
        return [
            copy(ext.at[pl.ds(HALO_BLK, HALO_BLK)], ext.at[pl.ds(HALO_BLK + blocks, HALO_BLK)], v_ss.at[0], v_rs.at[0], to(-1)),
            copy(ext.at[pl.ds(blocks, HALO_BLK)], ext.at[pl.ds(0, HALO_BLK)], v_ss.at[1], v_rs.at[1], to(1)),
        ]

    def rim_copy(k):
        return copy(rim.at[k], rim_in.at[k], c_ss.at[k], c_rs.at[k], to(OFFSETS[k]))

    def pot_copy(k):
        return copy(pot, pot_in.at[k], h_ss.at[k], h_rs.at[k], to(OFFSETS[k]))

    def f1_copies():
        out = []
        for d in far_first(nq):
            q, peer = q_peer(d)
            out.append(copy(f1_src.at[rows(q, nz)], f1_dst.at[rows(my_q, nz)], f1_ss.at[d], f1_rs.at[d], peer))
        return out

    def f2_copies():
        out = []
        for d in far_first(nz):
            z, peer = z_peer(d)
            out.append(copy(f2_src.at[rows(z, nq)], f2_dst.at[rows(my_z, nq)], f2_ss.at[d], f2_rs.at[d], peer))
        return out

    def a_copies():
        out = []
        for d in far_first(nz):
            z, peer = z_peer(d)
            out.append(copy(a_src.at[rows(z, nq)], a_dst.at[rows(my_z, nq)], a_ss.at[d], a_rs.at[d], peer))
        return out

    def b_copies():
        out = []
        for d in far_first(nq):
            q, peer = q_peer(d)
            out.append(copy(b_src.at[rows(q, nz)], b_dst.at[rows(my_q, nz)], b_ss.at[d], b_rs.at[d], peer))
        return out

    def spread(planes):
        v = vecs[M]
        for slot, p in enumerate(planes):
            value = x_spline[0, p : p + 1, :]
            slope = x_spline[1, p : p + 1, :]
            band = slice(slot * GRID, (slot + 1) * GRID)
            hi, lo = split(y_t[...] * (v[0:1] * slope) + dy_t[...] * (v[1:2] * value))
            lhs_hi[band, :atoms] = hi
            lhs_lo[band, :atoms] = lo
            hi, lo = split(y_t[...] * (v[2:3] * value))
            lhs_hi[band, atoms:] = hi
            lhs_lo[band, atoms:] = lo
        size = len(planes) * GRID
        wide = fast_dot(lhs_hi[:size, :], zz[...])
        return wide[:, :GRID] + wide[:, GRID:] + fast_dot(lhs_lo[:size, :], zz[:, :GRID])

    chunk = 32

    def pair_block(b, carry):
        v_rows, p_rows = [], []
        for e in range(2 * HALO_BLK + 1):
            tile = ext[b + e]
            shift = jnp.where(b + e < HALO_BLK, -1.0 * blocks, jnp.where(b + e >= HALO_BLK + blocks, 1.0 * blocks, 0.0)).astype(F32)
            v_rows.append(tile[0:3] * link[b, e])
            p_rows.append((tile[3:4] + shift, tile[4:5], tile[5:6]))

        def strip(i, inner):
            at_rows = pl.ds(pl.multiple_of(b * TILE + i * chunk, chunk), chunk)
            hx, hy, hz = home[0, at_rows, :], home[1, at_rows, :], home[2, at_rows, :]
            ax = jnp.zeros((chunk, TILE), F32)
            ay, az = ax, ax
            for e in range(2 * HALO_BLK + 1):
                px, py, pz = p_rows[e]
                vx, vy, vz = v_rows[e][0:1], v_rows[e][1:2], v_rows[e][2:3]
                dx, dy, dz = hx - px, hy - py, hz - pz
                inverse = lax.rsqrt(dx * dx + dy * dy + dz * dz + 1.0)
                inverse_sq = inverse * inverse
                third = inverse_sq * inverse
                along = (dx * vx + dy * vy + dz * vz) * (third * inverse_sq) * 3.0
                ax = ax + (third * vx - along * dx)
                ay = ay + (third * vy - along * dy)
                az = az + (third * vz - along * dz)
            pair_acc[0, at_rows, :] = ax
            pair_acc[1, at_rows, :] = ay
            pair_acc[2, at_rows, :] = az
            return inner

        lax.fori_loop(0, TILE // chunk, strip, 0)
        cols = rows(b, TILE)
        for c in range(3):
            near[c : c + 1, cols] = jnp.sum(pair_acc[c, cols, :].T, axis=0, keepdims=True)
        return carry

    def gather_chunk(g, carry):
        wide = 256
        cols = rows(g, wide)
        plain = fast_dot(pot3[...], zt3[:, cols])
        sa = jnp.zeros((GRID, wide), F32)
        sb = sa
        for p in range(ORDER):
            band = plain[p * GRID : (p + 1) * GRID]
            sa = sa + x_spline[1, p : p + 1, cols] * band
            sb = sb + x_spline[0, p : p + 1, cols] * band
        far[0:1, cols] = jnp.sum(sa * y_t[:, cols], axis=0, keepdims=True)
        far[1:2, cols] = jnp.sum(sb * dy_t[:, cols], axis=0, keepdims=True)
        tilted = fast_dot(pot3[...], zt3[:, pl.ds(pl.multiple_of(atoms + g * wide, wide), wide)])
        sc = jnp.zeros((GRID, wide), F32)
        for p in range(ORDER):
            sc = sc + x_spline[0, p : p + 1, cols] * tilted[p * GRID : (p + 1) * GRID]
        far[2:3, cols] = jnp.sum(sc * y_t[:, cols], axis=0, keepdims=True)
        return carry

    def put_plane(p, plane):
        hi, lo = split(plane)
        band = slice(p * GRID, (p + 1) * GRID)
        pot3[band, :GRID] = hi
        pot3[band, GRID : 2 * GRID] = lo
        pot3[band, 2 * GRID :] = hi

    def sweep(it, carry):
        v = vecs[M]
        for b in range(blocks):
            ext[HALO_BLK + b, 0:3, :] = v[:, b * TILE : (b + 1) * TILE]
        for c in vec_copies():
            c.start()
        for pair in ((0, 1), (2, 3)):
            both = spread([OFFSETS[k] + 2 for k in pair])
            for slot, k in enumerate(pair):
                rim[k] = both[slot * GRID : (slot + 1) * GRID]
                rim_copy(k).start()
        own = spread([2])
        for k in range(len(OFFSETS)):
            rim_copy(k).wait_recv()
            own = own + rim_in[k]
        along_z = exact_dot(own, four_t[...])
        f1_src[...] = exact_dot(four[...], along_z)
        for c in f1_copies():
            c.start()
        f1_dst[rows(my_q, nz), :] = f1_src[rows(my_q, nz), :]

        for c in vec_copies():
            c.wait_recv()
        lax.fori_loop(0, 2, pair_block, 0)

        @pl.when(it > 0)
        def _():
            reduce_middle()

        for c in f1_copies():
            c.wait_recv()
        for z in range(nz):
            f2_src[z * nq : (z + 1) * nq, :] = f1_dst[pl.ds(z, nq, stride=nz), :]
        for c in f2_copies():
            c.start()
        f2_dst[rows(my_z, nq), :] = f2_src[rows(my_z, nq), :]

        lax.fori_loop(2, blocks, pair_block, 0)

        @pl.when(it > 0)
        def _():
            reduce_end()

        for c in f2_copies():
            c.wait_recv()
        lines = exact_dot(four_x[...], f2_dst[...]) * green[...]
        a_src[...] = exact_dot(four_xt[...], lines)
        for c in a_copies():
            c.start()
        a_dst[rows(my_z, nq), :] = a_src[rows(my_z, nq), :]
        for c in a_copies():
            c.wait_recv()
        for q in range(nq):
            b_src[q * nz : (q + 1) * nz, :] = a_dst[pl.ds(q, nz, stride=nq), :]
        for c in b_copies():
            c.start()
        b_dst[rows(my_q, nz), :] = b_src[rows(my_q, nz), :]
        for c in b_copies():
            c.wait_recv()
        along_k = exact_dot(four_t[...], b_dst[...])
        mine = exact_dot(along_k, four[...])
        pot[...] = mine
        for k in range(len(OFFSETS)):
            pot_copy(k).start()
        put_plane(2, mine)
        for k in range(len(OFFSETS)):
            pot_copy(k).wait_recv()
            put_plane(2 - OFFSETS[k], pot_in[k])
        lax.fori_loop(0, atoms // 256, gather_chunk, 0)
        image = ip * v + far[...] - PAIR_C * (near[...] - v)

        @pl.when(it == 0)
        def _():
            vecs[W] = image

        @pl.when(it > 0)
        def _():
            gamma = scal[2, 0:1, 0:1]
            delta = scal[2, 1:2, 0:1]
            beta = jnp.where(it == 1, 0.0, gamma / scal[0, 0:1, 0:1])
            alpha = gamma / (delta - beta * gamma / scal[1, 0:1, 0:1])
            scal[0] = jnp.broadcast_to(gamma, (8, TILE))
            scal[1] = jnp.broadcast_to(alpha, (8, TILE))
            new_z = image + beta * vecs[Z]
            new_q = v + beta * vecs[Q]
            new_s = vecs[W] + beta * vecs[S]
            new_p = vecs[U] + beta * vecs[PP]
            vecs[Z] = new_z
            vecs[Q] = new_q
            vecs[S] = new_s
            vecs[PP] = new_p
            vecs[X] = vecs[X] + alpha * new_p
            vecs[R] = vecs[R] - alpha * new_s
            vecs[U] = vecs[U] - alpha * new_q
            vecs[W] = vecs[W] - alpha * new_z

        reduce_start()
        vecs[M] = vecs[W] / ip
        for group in (vec_copies(), f1_copies(), f2_copies(), a_copies(), b_copies()):
            for c in group:
                c.wait_send()
        for k in range(len(OFFSETS)):
            rim_copy(k).wait_send()
            pot_copy(k).wait_send()
        return carry

    lax.fori_loop(0, ITERS, sweep, 0)
    reduce_middle()
    reduce_end()
    gamma = scal[2, 0:1, 0:1]
    delta = scal[2, 1:2, 0:1]
    beta = gamma / scal[0, 0:1, 0:1]
    alpha = gamma / (delta - beta * gamma / scal[1, 0:1, 0:1])
    dip_out[...] = vecs[X] + alpha * (vecs[U] + beta * vecs[PP])
    res_out[...] = vecs[R] - alpha * (vecs[W] + beta * vecs[S])


def per_device(n, positions, field, inv_polar, x_spline, yz_spline, tile_list, tile_count):
    atoms = positions.shape[1]
    blocks = atoms // TILE
    nq = NX * NC
    nz = n // nq
    rows_x = np.arange(GRID)
    q, z = rows_x % nq, rows_x // nq
    plane = (q // NC) * (nz * NC) + z * NC + q % NC
    table = basis(GRID)
    four = jnp.asarray(table, F32)
    four_t = jnp.asarray(table.T.copy(), F32)
    four_x = jnp.asarray(table[:, plane], F32)
    four_xt = jnp.asarray(table[:, plane].T.copy(), F32)
    vm = pl.BlockSpec(memory_space=pltpu.VMEM)
    sm = pl.BlockSpec(memory_space=pltpu.SMEM)
    square = pltpu.VMEM((GRID, GRID), F32)
    sem = pltpu.SemaphoreType.DMA
    out = jax.ShapeDtypeStruct((3, atoms), F32)
    return pl.pallas_call(
        functools.partial(solve_kernel, n),
        out_shape=(out, out),
        in_specs=[sm, sm] + [vm] * 9,
        out_specs=(vm, vm),
        scratch_shapes=[
            pltpu.SMEM((blocks, 2 * HALO_BLK + 1), F32),
            pltpu.VMEM((blocks + 2 * HALO_BLK, 8, TILE), F32),
            pltpu.VMEM((3, atoms, TILE), F32),
            pltpu.VMEM((3, atoms, TILE), F32),
            pltpu.VMEM((3, atoms), F32),
            pltpu.VMEM((3, atoms), F32),
            pltpu.VMEM((GRID, atoms), F32),
            pltpu.VMEM((GRID, atoms), F32),
            pltpu.VMEM((2 * atoms, 2 * GRID), BF16),
            pltpu.VMEM((3 * GRID, 2 * atoms), BF16),
            pltpu.VMEM((2 * GRID, 2 * atoms), BF16),
            pltpu.VMEM((2 * GRID, 2 * atoms), BF16),
            pltpu.VMEM((4, GRID, GRID), F32),
            pltpu.VMEM((4, GRID, GRID), F32),
            square,
            pltpu.VMEM((4, GRID, GRID), F32),
            pltpu.VMEM((ORDER * GRID, 3 * GRID), BF16),
            square,
            square, square, square, square,
            square, square, square, square,
            pltpu.VMEM((8, TILE), F32),
            pltpu.VMEM((nz, 8, TILE), F32),
            pltpu.VMEM((8, TILE), F32),
            pltpu.VMEM((nq, 8, TILE), F32),
            pltpu.VMEM((9, 3, atoms), F32),
            pltpu.VMEM((3, 8, TILE), F32),
            sem((2,)), sem((2,)),
            sem((4,)), sem((4,)),
            sem((4,)), sem((4,)),
            sem((nq,)), sem((nq,)),
            sem((nz,)), sem((nz,)),
            sem((nz,)), sem((nz,)),
            sem((nq,)), sem((nq,)),
            sem((nz,)), sem((nz,)),
            sem((nq,)), sem((nq,)),
        ],
        compiler_params=pltpu.CompilerParams(
            collective_id=0, has_side_effects=True, vmem_limit_bytes=56 * 1024 * 1024
        ),
    )(tile_list, tile_count, positions, field, inv_polar.reshape(1, atoms), x_spline, yz_spline,
      four, four_t, four_x, four_xt)


def solution(mesh):
    both = ("rep", "gx")
    in_specs = (
        P(None, both),
        P(None, both),
        P(both),
        P(None, None, both),
        P(None, both, None),
        P(both, None),
        P(both),
    )
    out_specs = (P(None, both), P(None, both))
    return jax.shard_map(
        functools.partial(per_device, mesh.shape["gx"]),
        mesh=mesh, in_specs=in_specs, out_specs=out_specs, check_vma=False,
    )
```

```python
import functools

import jax
import jax.numpy as jnp
import numpy as np
from jax import lax
from jax.experimental import pallas as pl
from jax.experimental.pallas import tpu as pltpu
from jax.sharding import PartitionSpec as P

GRID = 128
ORDER = 5
TILE = 128
HALO_BLK = 3
ITERS = 3
PAIR_C = 0.025
RECIP_C = 8192.0
DAMP = 0.0008
EXACT = lax.Precision.HIGHEST
MESH = pl.DeviceIdType.MESH
F32 = jnp.float32
BF16 = jnp.bfloat16
NX = 4
NC = 2
OFFSETS = (-2, 2, -1, 1)


def far_first(count):
    return sorted(range(1, count), key=lambda d: -min(d, count - d))


def basis(size):
    freq = np.arange(size)
    half = size // 2
    mode = np.where(freq <= half, freq, freq - half)
    angle = (mode[:, None] * np.arange(size)[None, :] % size) * (2.0 * np.pi / size)
    return np.where((freq <= half)[:, None], np.cos(angle), np.sin(angle))


def split(x):
    hi = x.astype(BF16)
    return hi, (x - hi.astype(F32)).astype(BF16)


def exact_dot(a, b):
    return jnp.dot(a, b, precision=EXACT, preferred_element_type=F32)


def fast_dot(a, b):
    return jnp.dot(a, b, preferred_element_type=F32)


def mode_of(freq, size):
    half = size // 2
    mode = jnp.where(freq <= half, freq, freq - half)
    weight = jnp.where((freq == 0) | (freq == half), 1.0 / size, 2.0 / size)
    return mode.astype(F32), weight.astype(F32)


def solve_kernel(
    n,
    tile_list,
    tile_count,
    pos,
    field,
    inv_polar,
    x_spline,
    yz,
    four,
    four_t,
    four_x,
    four_xt,
    dip_a,
    dip_b,
    res_a,
    res_b,
    step_out,
    link,
    ext,
    home,
    pair_acc,
    near,
    far,
    y_t,
    dy_t,
    zz,
    zt4,
    lhs_hi,
    lhs_lo,
    rim,
    rim_in,
    own_plane,
    pot,
    pot_in,
    pot4,
    green,
    f1_src,
    f1_dst,
    f2_src,
    f2_dst,
    a_src,
    a_dst,
    b_src,
    b_dst,
    ra_src,
    ra_dst,
    rb_src,
    rb_dst,
    vecs,
    scal,
    v_ss,
    v_rs,
    c_ss,
    c_rs,
    h_ss,
    h_rs,
    f1_ss,
    f1_rs,
    f2_ss,
    f2_rs,
    a_ss,
    a_rs,
    b_ss,
    b_rs,
    ra_ss,
    ra_rs,
    rb_ss,
    rb_rs,
):
    nq = NX * NC
    nz = n // nq
    me = lax.axis_index("gx")
    my_q = (me // (nz * NC)) * NC + me % NC
    my_z = me % (nz * NC) // NC
    blocks = pos.shape[1] // TILE
    atoms = pos.shape[1]

    def at(q, z):
        return (q // NC) * (nz * NC) + z * NC + q % NC

    def q_peer(d):
        q = (my_q + d) % nq
        return q, at(q, my_z)

    def z_peer(d):
        z = (my_z + d) % nz
        return z, at(my_q, z)

    def to(d):
        return (me + d + n) % n

    def copy(src, dst, ss, rs, peer):
        return pltpu.make_async_remote_copy(
            src_ref=src, dst_ref=dst, send_sem=ss, recv_sem=rs,
            device_id={"gx": peer}, device_id_type=MESH,
        )

    def rows(i, size):
        return pl.ds(pl.multiple_of(i * size, size), size)

    barrier = pltpu.get_barrier_semaphore()
    for d in far_first(nz):
        pl.semaphore_signal(barrier, inc=1, device_id={"gx": z_peer(d)[1]}, device_id_type=MESH)
    for d in far_first(nq):
        pl.semaphore_signal(barrier, inc=1, device_id={"gx": q_peer(d)[1]}, device_id_type=MESH)
    for d in OFFSETS:
        pl.semaphore_signal(barrier, inc=1, device_id={"gx": to(d)}, device_id_type=MESH)

    def prepare(b, carry):
        cols = rows(b, TILE)
        y_t[:, cols] = yz[0, cols, :].T
        dy_t[:, cols] = yz[1, cols, :].T
        for part in range(2):
            hi, lo = split(yz[2 + part, cols, :])
            at_rows = pl.ds(pl.multiple_of(part * atoms + b * TILE, TILE), TILE)
            zz[at_rows, :GRID] = hi
            zz[at_rows, GRID:] = lo
        ext[HALO_BLK + b, 3:6, :] = pos[:, cols]
        return carry

    def prepare_more(b, carry):
        cols = rows(b, TILE)
        for part in range(2):
            at_rows = pl.ds(pl.multiple_of(part * atoms + b * TILE, TILE), TILE)
            hi, lo = split(yz[2 + part, cols, :].T)
            zt4[:GRID, at_rows] = hi
            zt4[GRID : 2 * GRID, at_rows] = hi
            zt4[2 * GRID : 3 * GRID, at_rows] = lo
            zt4[3 * GRID :, at_rows] = lo
        here = pos[:, cols]
        for c in range(3):
            home[c, cols, :] = jnp.broadcast_to(here[c : c + 1], (TILE, TILE)).T
        for e in range(2 * HALO_BLK + 1):
            total = jnp.float32(0.0)
            for k in range(tile_list.shape[1]):
                hit = (tile_list[b, k] == b + e) & (k < tile_count[b])
                total = total + jnp.where(hit, jnp.float32(1.0), jnp.float32(0.0))
            link[b, e] = total
        return carry

    def prepare_green():
        row_freq = lax.broadcasted_iota(jnp.int32, (GRID, GRID), 0)
        col_freq = lax.broadcasted_iota(jnp.int32, (GRID, GRID), 1)
        kx, wx = mode_of(row_freq, GRID)
        kz, wz = mode_of(col_freq, GRID)
        ky, wy = mode_of(jnp.full((GRID, GRID), my_q * nz + my_z, jnp.int32), GRID)
        mode_sq = kx * kx + ky * ky + kz * kz
        safe_sq = jnp.where(mode_sq > 0, mode_sq, 1.0)
        green[...] = jnp.where(mode_sq > 0, RECIP_C * jnp.exp(-DAMP * safe_sq) / safe_sq, 0.0) * wx * wy * wz

    ip = inv_polar[...]
    R, U, PP, S, X = range(5)

    def reduce_a():
        return [copy(ra_src, ra_dst.at[my_z], ra_ss.at[d], ra_rs.at[d], z_peer(d)[1]) for d in far_first(nz)]

    def reduce_b():
        return [copy(rb_src, rb_dst.at[my_q], rb_ss.at[d], rb_rs.at[d], q_peer(d)[1]) for d in far_first(nq)]

    def folded(value):
        lanes = sum(value[:, k * TILE : (k + 1) * TILE] for k in range(atoms // TILE))
        return jnp.sum(lanes, axis=0, keepdims=True)

    def reduce_start(energy):
        u = vecs[U]
        ra_src[0:1, :] = folded(vecs[R] * u)
        ra_src[1:2, :] = folded((ip * u - PAIR_C * (near[...] - u)) * u) + energy
        ra_dst[my_z] = ra_src[...]
        for c in reduce_a():
            c.start()

    def reduce_middle():
        for c in reduce_a():
            c.wait_recv()
        rb_src[...] = jnp.sum(ra_dst[...], axis=0)
        rb_dst[my_q] = rb_src[...]
        for c in reduce_b():
            c.start()

    def reduce_end():
        for c in reduce_b():
            c.wait_recv()
        sums = jnp.sum(jnp.sum(rb_dst[...], axis=0), axis=1, keepdims=True)
        for c in reduce_a():
            c.wait_send()
        for c in reduce_b():
            c.wait_send()
        return sums[0:1], sums[1:2]

    def vec_copies():
        return [
            copy(ext.at[pl.ds(HALO_BLK, HALO_BLK)], ext.at[pl.ds(HALO_BLK + blocks, HALO_BLK)], v_ss.at[0], v_rs.at[0], to(-1)),
            copy(ext.at[pl.ds(blocks, HALO_BLK)], ext.at[pl.ds(0, HALO_BLK)], v_ss.at[1], v_rs.at[1], to(1)),
        ]

    def rim_copy(k):
        return copy(rim.at[k], rim_in.at[k], c_ss.at[k], c_rs.at[k], to(OFFSETS[k]))

    def pot_copy(k):
        return copy(pot, pot_in.at[k], h_ss.at[k], h_rs.at[k], to(OFFSETS[k]))

    def f1_copies():
        out = []
        for d in far_first(nq):
            q, peer = q_peer(d)
            out.append(copy(f1_src.at[rows(q, nz)], f1_dst.at[rows(my_q, nz)], f1_ss.at[d], f1_rs.at[d], peer))
        return out

    def f2_copies():
        out = []
        for d in far_first(nz):
            z, peer = z_peer(d)
            out.append(copy(f2_src.at[rows(z, nq)], f2_dst.at[rows(my_z, nq)], f2_ss.at[d], f2_rs.at[d], peer))
        return out

    def a_copies():
        out = []
        for d in far_first(nz):
            z, peer = z_peer(d)
            out.append(copy(a_src.at[rows(z, nq)], a_dst.at[rows(my_z, nq)], a_ss.at[d], a_rs.at[d], peer))
        return out

    def b_copies():
        out = []
        for d in far_first(nq):
            q, peer = q_peer(d)
            out.append(copy(b_src.at[rows(q, nz)], b_dst.at[rows(my_q, nz)], b_ss.at[d], b_rs.at[d], peer))
        return out

    def spread(planes):
        v = vecs[U]
        for slot, p in enumerate(planes):
            value = x_spline[p, 0:1, :]
            slope = x_spline[p, 1:2, :]
            band = slice(slot * GRID, (slot + 1) * GRID)
            hi, lo = split(y_t[...] * (v[0:1] * slope) + dy_t[...] * (v[1:2] * value))
            lhs_hi[band, :atoms] = hi
            lhs_lo[band, :atoms] = lo
            hi, lo = split(y_t[...] * (v[2:3] * value))
            lhs_hi[band, atoms:] = hi
            lhs_lo[band, atoms:] = lo
        size = len(planes) * GRID
        wide = fast_dot(lhs_hi[:size, :], zz[...]) + fast_dot(lhs_lo[:size, :], zz[...])
        return wide[:, :GRID] + wide[:, GRID:]

    chunk = 32

    def pair_block(b, carry):
        v_rows, p_rows = [], []
        for e in range(2 * HALO_BLK + 1):
            tile = ext[b + e]
            shift = jnp.where(b + e < HALO_BLK, -1.0 * blocks, jnp.where(b + e >= HALO_BLK + blocks, 1.0 * blocks, 0.0)).astype(F32)
            v_rows.append(tile[0:3] * link[b, e])
            p_rows.append((tile[3:4] + shift, tile[4:5], tile[5:6]))

        def strip(i, inner):
            at_rows = pl.ds(pl.multiple_of(b * TILE + i * chunk, chunk), chunk)
            hx, hy, hz = home[0, at_rows, :], home[1, at_rows, :], home[2, at_rows, :]
            ax = jnp.zeros((chunk, TILE), F32)
            ay, az = ax, ax
            for e in range(2 * HALO_BLK + 1):
                px, py, pz = p_rows[e]
                vx, vy, vz = v_rows[e][0:1], v_rows[e][1:2], v_rows[e][2:3]
                dx, dy, dz = hx - px, hy - py, hz - pz
                inverse = lax.rsqrt(dx * dx + dy * dy + dz * dz + 1.0)
                inverse_sq = inverse * inverse
                third = inverse_sq * inverse
                along = (dx * vx + dy * vy + dz * vz) * (third * inverse_sq) * 3.0
                ax = ax + (third * vx - along * dx)
                ay = ay + (third * vy - along * dy)
                az = az + (third * vz - along * dz)
            pair_acc[0, at_rows, :] = ax
            pair_acc[1, at_rows, :] = ay
            pair_acc[2, at_rows, :] = az
            return inner

        lax.fori_loop(0, TILE // chunk, strip, 0)
        cols = rows(b, TILE)
        for c in range(3):
            near[c : c + 1, cols] = jnp.sum(pair_acc[c, cols, :].T, axis=0, keepdims=True)
        return carry

    def gather_chunk(g, carry):
        wide = 256
        cols = rows(g, wide)
        plain = fast_dot(pot4[...], zt4[:, cols])
        sa = jnp.zeros((GRID, wide), F32)
        sb = sa
        for p in range(ORDER):
            band = plain[p * GRID : (p + 1) * GRID]
            sa = sa + x_spline[p, 1:2, cols] * band
            sb = sb + x_spline[p, 0:1, cols] * band
        far[0:1, cols] = jnp.sum(sa * y_t[:, cols], axis=0, keepdims=True)
        far[1:2, cols] = jnp.sum(sb * dy_t[:, cols], axis=0, keepdims=True)
        tilted = fast_dot(pot4[...], zt4[:, pl.ds(pl.multiple_of(atoms + g * wide, wide), wide)])
        sc = jnp.zeros((GRID, wide), F32)
        for p in range(ORDER):
            sc = sc + x_spline[p, 0:1, cols] * tilted[p * GRID : (p + 1) * GRID]
        far[2:3, cols] = jnp.sum(sc * y_t[:, cols], axis=0, keepdims=True)
        return carry

    def put_plane(p, plane):
        hi, lo = split(plane)
        band = slice(p * GRID, (p + 1) * GRID)
        pot4[band, :GRID] = hi
        pot4[band, GRID : 2 * GRID] = lo
        pot4[band, 2 * GRID : 3 * GRID] = hi
        pot4[band, 3 * GRID :] = lo

    def put_vector():
        v = vecs[U]
        for b in range(blocks):
            ext[HALO_BLK + b, 0:3, :] = v[:, b * TILE : (b + 1) * TILE]

    def spread_pair(pair):
        both = spread([OFFSETS[k] + 2 for k in pair])
        for slot, k in enumerate(pair):
            rim[k] = both[slot * GRID : (slot + 1) * GRID]

    lax.fori_loop(0, blocks, prepare, 0)
    vecs[R] = field[...]
    vecs[U] = field[...] / ip
    for name in (PP, S, X):
        vecs[name] = jnp.zeros((3, atoms), F32)
    scal[...] = jnp.ones_like(scal)
    ra_src[...] = jnp.zeros_like(ra_src)
    put_vector()
    spread_pair((0, 1))
    spread_pair((2, 3))
    pl.semaphore_wait(barrier, (nz - 1) + (nq - 1) + len(OFFSETS))
    for k in range(len(OFFSETS)):
        rim_copy(k).start()
    for c in vec_copies():
        c.start()
    own_plane[...] = spread([2])

    def sweep(it, carry):
        own = own_plane[...]
        for k in range(len(OFFSETS)):
            rim_copy(k).wait_recv()
            own = own + rim_in[k]
        along_z = exact_dot(own, four_t[...])
        f1_src[...] = exact_dot(four[...], along_z)
        for c in f1_copies():
            c.start()
        f1_dst[rows(my_q, nz), :] = f1_src[rows(my_q, nz), :]

        @pl.when(it == 0)
        def _():
            lax.fori_loop(0, blocks, prepare_more, 0)
            prepare_green()

        for c in vec_copies():
            c.wait_recv()
        lax.fori_loop(0, 2, pair_block, 0)

        for c in f1_copies():
            c.wait_recv()
        for z in range(nz):
            f2_src[z * nq : (z + 1) * nq, :] = f1_dst[pl.ds(z, nq, stride=nz), :]
        for c in f2_copies():
            c.start()
        f2_dst[rows(my_z, nq), :] = f2_src[rows(my_z, nq), :]

        lax.fori_loop(2, blocks, pair_block, 0)

        for c in f2_copies():
            c.wait_recv()
        lines = exact_dot(four_x[...], f2_dst[...])
        scaled = lines * green[...]
        a_src[...] = exact_dot(four_xt[...], scaled)
        for c in a_copies():
            c.start()
        a_dst[rows(my_z, nq), :] = a_src[rows(my_z, nq), :]
        reduce_start(jnp.sum(lines * scaled, axis=0, keepdims=True))
        for c in a_copies():
            c.wait_recv()
        for q in range(nq):
            b_src[q * nz : (q + 1) * nz, :] = a_dst[pl.ds(q, nz, stride=nq), :]
        for c in b_copies():
            c.start()
        b_dst[rows(my_q, nz), :] = b_src[rows(my_q, nz), :]
        reduce_middle()
        for c in b_copies():
            c.wait_recv()
        along_k = exact_dot(four_t[...], b_dst[...])
        mine = exact_dot(along_k, four[...])
        pot[...] = mine
        for k in (2, 3, 0, 1):
            pot_copy(k).start()
        put_plane(2, mine)
        for group in (vec_copies(), f1_copies(), f2_copies(), a_copies(), b_copies()):
            for c in group:
                c.wait_send()
        for k in range(len(OFFSETS)):
            rim_copy(k).wait_send()
        for k in (2, 3, 0, 1):
            pot_copy(k).wait_recv()
            put_plane(2 - OFFSETS[k], pot_in[k])
        lax.fori_loop(0, atoms // 256, gather_chunk, 0)
        u = vecs[U]
        image = ip * u + far[...] - PAIR_C * (near[...] - u)
        gamma, delta = reduce_end()
        beta = jnp.where(it == 0, 0.0, gamma / scal[0, 0:1, 0:1])
        alpha = gamma / (delta - beta * gamma / scal[1, 0:1, 0:1])
        scal[0] = jnp.broadcast_to(gamma, (8, TILE))
        scal[1] = jnp.broadcast_to(alpha, (8, TILE))
        new_p = u + beta * vecs[PP]
        new_s = image + beta * vecs[S]
        vecs[PP] = new_p
        vecs[S] = new_s

        @pl.when(it < ITERS - 1)
        def _():
            residual = vecs[R] - alpha * new_s
            vecs[U] = residual / ip
            put_vector()
            for c in vec_copies():
                c.start()
            vecs[R] = residual
            vecs[X] = vecs[X] + alpha * new_p
            for pair in ((0, 1), (2, 3)):
                spread_pair(pair)
                for k in pair:
                    rim_copy(k).start()
            own_plane[...] = spread([2])

        @pl.when(it == ITERS - 1)
        def _():
            dip_a[...] = vecs[X]
            dip_b[...] = new_p
            step_out[...] = jnp.broadcast_to(alpha, (3, atoms))
            res_a[...] = vecs[R]
            res_b[...] = new_s

        for k in range(len(OFFSETS)):
            pot_copy(k).wait_send()
        return carry

    lax.fori_loop(0, ITERS, sweep, 0)


def per_device(n, positions, field, inv_polar, x_spline, yz_spline, tile_list, tile_count):
    atoms = positions.shape[1]
    blocks = atoms // TILE
    nq = NX * NC
    nz = n // nq
    rows_x = np.arange(GRID)
    q, z = rows_x % nq, rows_x // nq
    plane = (q // NC) * (nz * NC) + z * NC + q % NC
    table = basis(GRID)
    four = jnp.asarray(table, F32)
    four_t = jnp.asarray(table.T.copy(), F32)
    four_x = jnp.asarray(table[:, plane], F32)
    four_xt = jnp.asarray(table[:, plane].T.copy(), F32)
    vm = pl.BlockSpec(memory_space=pltpu.VMEM)
    sm = pl.BlockSpec(memory_space=pltpu.SMEM)
    square = pltpu.VMEM((GRID, GRID), F32)
    sem = pltpu.SemaphoreType.DMA
    out = jax.ShapeDtypeStruct((3, atoms), F32)
    dip_a, dip_b, res_a, res_b, step = pl.pallas_call(
        functools.partial(solve_kernel, n),
        out_shape=(out,) * 5,
        in_specs=[sm, sm] + [vm] * 9,
        out_specs=(vm,) * 5,
        scratch_shapes=[
            pltpu.SMEM((blocks, 2 * HALO_BLK + 1), F32),
            pltpu.VMEM((blocks + 2 * HALO_BLK, 8, TILE), F32),
            pltpu.VMEM((3, atoms, TILE), F32),
            pltpu.VMEM((3, atoms, TILE), F32),
            pltpu.VMEM((3, atoms), F32),
            pltpu.VMEM((3, atoms), F32),
            pltpu.VMEM((GRID, atoms), F32),
            pltpu.VMEM((GRID, atoms), F32),
            pltpu.VMEM((2 * atoms, 2 * GRID), BF16),
            pltpu.VMEM((4 * GRID, 2 * atoms), BF16),
            pltpu.VMEM((2 * GRID, 2 * atoms), BF16),
            pltpu.VMEM((2 * GRID, 2 * atoms), BF16),
            pltpu.VMEM((4, GRID, GRID), F32),
            pltpu.VMEM((4, GRID, GRID), F32),
            square,
            square,
            pltpu.VMEM((4, GRID, GRID), F32),
            pltpu.VMEM((ORDER * GRID, 4 * GRID), BF16),
            square,
            square, square, square, square,
            square, square, square, square,
            pltpu.VMEM((8, TILE), F32),
            pltpu.VMEM((nz, 8, TILE), F32),
            pltpu.VMEM((8, TILE), F32),
            pltpu.VMEM((nq, 8, TILE), F32),
            pltpu.VMEM((5, 3, atoms), F32),
            pltpu.VMEM((2, 8, TILE), F32),
            sem((2,)), sem((2,)),
            sem((4,)), sem((4,)),
            sem((4,)), sem((4,)),
            sem((nq,)), sem((nq,)),
            sem((nz,)), sem((nz,)),
            sem((nz,)), sem((nz,)),
            sem((nq,)), sem((nq,)),
            sem((nz,)), sem((nz,)),
            sem((nq,)), sem((nq,)),
        ],
        compiler_params=pltpu.CompilerParams(
            collective_id=0, has_side_effects=True, vmem_limit_bytes=56 * 1024 * 1024
        ),
    )(tile_list, tile_count, positions, field, inv_polar.reshape(1, atoms), x_spline.transpose(1, 0, 2), yz_spline,
      four, four_t, four_x, four_xt)
    return dip_a + step * dip_b, res_a - step * res_b


def solution(mesh):
    both = ("rep", "gx")
    in_specs = (
        P(None, both),
        P(None, both),
        P(both),
        P(None, None, both),
        P(None, both, None),
        P(both, None),
        P(both),
    )
    out_specs = (P(None, both), P(None, both))
    return jax.shard_map(
        functools.partial(per_device, mesh.shape["gx"]),
        mesh=mesh, in_specs=in_specs, out_specs=out_specs, check_vma=False,
    )
```

```python
import functools

import jax
import jax.numpy as jnp
import numpy as np
from jax import lax
from jax.experimental import pallas as pl
from jax.experimental.pallas import tpu as pltpu
from jax.sharding import PartitionSpec as P

GRID = 128
ORDER = 5
TILE = 128
HALO_BLK = 3
ITERS = 3
PAIR_C = 0.025
RECIP_C = 8192.0
DAMP = 0.0008
MESH = pl.DeviceIdType.MESH
F32 = jnp.float32
BF16 = jnp.bfloat16
NX = 4
NC = 2
OFFSETS = (-2, 2, -1, 1)


def far_first(count):
    return sorted(range(1, count), key=lambda d: -min(d, count - d))


def basis(size):
    freq = np.arange(size)
    half = size // 2
    mode = np.where(freq <= half, freq, freq - half)
    angle = (mode[:, None] * np.arange(size)[None, :] % size) * (2.0 * np.pi / size)
    return np.where((freq <= half)[:, None], np.cos(angle), np.sin(angle))


def split(x):
    hi = x.astype(BF16)
    return hi, (x - hi.astype(F32)).astype(BF16)


def left_dot(stacked, x):
    hi, lo = split(x)
    return fast_dot(stacked[...], jnp.concatenate([hi, hi, lo], axis=0))


def right_dot(x, stacked):
    hi, lo = split(x)
    return fast_dot(jnp.concatenate([hi, lo, hi], axis=1), stacked[...])


def fast_dot(a, b):
    return jnp.dot(a, b, preferred_element_type=F32)


def mode_of(freq, size):
    half = size // 2
    mode = jnp.where(freq <= half, freq, freq - half)
    weight = jnp.where((freq == 0) | (freq == half), 1.0 / size, 2.0 / size)
    return mode.astype(F32), weight.astype(F32)


def solve_kernel(
    n,
    tile_list,
    tile_count,
    pos,
    field,
    inv_polar,
    x_spline,
    yz_hbm,
    fwd_right,
    fwd_left,
    x_left,
    xt_left,
    inv_left,
    inv_right,
    dip_a,
    dip_b,
    res_a,
    res_b,
    step_out,
    yz,
    yz_sem,
    link,
    ext,
    home,
    pair_acc,
    near,
    far,
    y_t,
    dy_t,
    zz,
    zt3,
    lhs_hi,
    lhs_lo,
    rim,
    rim_in,
    own_plane,
    pot,
    pot_in,
    pot3,
    green,
    f1_src,
    f1_dst,
    f2_src,
    f2_dst,
    a_src,
    a_dst,
    b_src,
    b_dst,
    ra_src,
    ra_dst,
    rb_src,
    rb_dst,
    vecs,
    scal,
    v_ss,
    v_rs,
    c_ss,
    c_rs,
    h_ss,
    h_rs,
    f1_ss,
    f1_rs,
    f2_ss,
    f2_rs,
    a_ss,
    a_rs,
    b_ss,
    b_rs,
    ra_ss,
    ra_rs,
    rb_ss,
    rb_rs,
):
    nq = NX * NC
    nz = n // nq
    me = lax.axis_index("gx")
    my_q = (me // (nz * NC)) * NC + me % NC
    my_z = me % (nz * NC) // NC
    blocks = pos.shape[1] // TILE
    atoms = pos.shape[1]

    def at(q, z):
        return (q // NC) * (nz * NC) + z * NC + q % NC

    def q_peer(d):
        q = (my_q + d) % nq
        return q, at(q, my_z)

    def z_peer(d):
        z = (my_z + d) % nz
        return z, at(my_q, z)

    def to(d):
        return (me + d + n) % n

    def copy(src, dst, ss, rs, peer):
        return pltpu.make_async_remote_copy(
            src_ref=src, dst_ref=dst, send_sem=ss, recv_sem=rs,
            device_id={"gx": peer}, device_id_type=MESH,
        )

    def rows(i, size):
        return pl.ds(pl.multiple_of(i * size, size), size)

    yz_copy = pltpu.make_async_copy(yz_hbm, yz, yz_sem)
    yz_copy.start()

    barrier = pltpu.get_barrier_semaphore()
    for d in far_first(nz):
        pl.semaphore_signal(barrier, inc=1, device_id={"gx": z_peer(d)[1]}, device_id_type=MESH)
    for d in far_first(nq):
        pl.semaphore_signal(barrier, inc=1, device_id={"gx": q_peer(d)[1]}, device_id_type=MESH)
    for d in OFFSETS:
        pl.semaphore_signal(barrier, inc=1, device_id={"gx": to(d)}, device_id_type=MESH)

    def prepare(b, carry):
        cols = rows(b, TILE)
        y_t[:, cols] = yz[0, cols, :].T
        dy_t[:, cols] = yz[1, cols, :].T
        for part in range(2):
            hi, lo = split(yz[2 + part, cols, :])
            at_rows = pl.ds(pl.multiple_of(part * atoms + b * TILE, TILE), TILE)
            zz[at_rows, :GRID] = hi
            zz[at_rows, GRID:] = lo
        ext[HALO_BLK + b, 3:6, :] = pos[:, cols]
        return carry

    def prepare_more(b, carry):
        cols = rows(b, TILE)
        for part in range(2):
            at_rows = pl.ds(pl.multiple_of(part * atoms + b * TILE, TILE), TILE)
            hi, lo = split(yz[2 + part, cols, :].T)
            zt3[:GRID, at_rows] = hi
            zt3[GRID : 2 * GRID, at_rows] = hi
            zt3[2 * GRID :, at_rows] = lo
        here = pos[:, cols]
        for c in range(3):
            home[c, cols, :] = jnp.broadcast_to(here[c : c + 1], (TILE, TILE)).T
        for e in range(2 * HALO_BLK + 1):
            total = jnp.float32(0.0)
            for k in range(tile_list.shape[1]):
                hit = (tile_list[b, k] == b + e) & (k < tile_count[b])
                total = total + jnp.where(hit, jnp.float32(1.0), jnp.float32(0.0))
            link[b, e] = total
        return carry

    def prepare_green():
        row_freq = lax.broadcasted_iota(jnp.int32, (GRID, GRID), 0)
        col_freq = lax.broadcasted_iota(jnp.int32, (GRID, GRID), 1)
        kx, wx = mode_of(row_freq, GRID)
        kz, wz = mode_of(col_freq, GRID)
        ky, wy = mode_of(jnp.full((GRID, GRID), my_q * nz + my_z, jnp.int32), GRID)
        mode_sq = kx * kx + ky * ky + kz * kz
        safe_sq = jnp.where(mode_sq > 0, mode_sq, 1.0)
        green[...] = jnp.where(mode_sq > 0, RECIP_C * jnp.exp(-DAMP * safe_sq) / safe_sq, 0.0) * wx * wy * wz

    ip = inv_polar[...]
    R, U, PP, S, X = range(5)

    def reduce_a():
        return [copy(ra_src, ra_dst.at[my_z], ra_ss.at[d], ra_rs.at[d], z_peer(d)[1]) for d in far_first(nz)]

    def reduce_b():
        return [copy(rb_src, rb_dst.at[my_q], rb_ss.at[d], rb_rs.at[d], q_peer(d)[1]) for d in far_first(nq)]

    def folded(value):
        lanes = sum(value[:, k * TILE : (k + 1) * TILE] for k in range(atoms // TILE))
        return jnp.sum(lanes, axis=0, keepdims=True)

    def reduce_start(energy):
        u = vecs[U]
        ra_src[0:1, :] = folded(vecs[R] * u)
        ra_src[1:2, :] = folded((ip * u - PAIR_C * (near[...] - u)) * u) + energy
        ra_dst[my_z] = ra_src[...]
        for c in reduce_a():
            c.start()

    def reduce_middle():
        for c in reduce_a():
            c.wait_recv()
        rb_src[...] = jnp.sum(ra_dst[...], axis=0)
        rb_dst[my_q] = rb_src[...]
        for c in reduce_b():
            c.start()

    def reduce_end():
        for c in reduce_b():
            c.wait_recv()
        sums = jnp.sum(jnp.sum(rb_dst[...], axis=0), axis=1, keepdims=True)
        for c in reduce_a():
            c.wait_send()
        for c in reduce_b():
            c.wait_send()
        return sums[0:1], sums[1:2]

    def vec_copies():
        return [
            copy(ext.at[pl.ds(HALO_BLK, HALO_BLK)], ext.at[pl.ds(HALO_BLK + blocks, HALO_BLK)], v_ss.at[0], v_rs.at[0], to(-1)),
            copy(ext.at[pl.ds(blocks, HALO_BLK)], ext.at[pl.ds(0, HALO_BLK)], v_ss.at[1], v_rs.at[1], to(1)),
        ]

    def rim_copy(k):
        return copy(rim.at[k], rim_in.at[k], c_ss.at[k], c_rs.at[k], to(OFFSETS[k]))

    def pot_copy(k):
        return copy(pot, pot_in.at[k], h_ss.at[k], h_rs.at[k], to(OFFSETS[k]))

    def f1_copies():
        out = []
        for d in far_first(nq):
            q, peer = q_peer(d)
            out.append(copy(f1_src.at[rows(q, nz)], f1_dst.at[rows(my_q, nz)], f1_ss.at[d], f1_rs.at[d], peer))
        return out

    def f2_copies():
        out = []
        for d in far_first(nz):
            z, peer = z_peer(d)
            out.append(copy(f2_src.at[rows(z, nq)], f2_dst.at[rows(my_z, nq)], f2_ss.at[d], f2_rs.at[d], peer))
        return out

    def a_copies():
        out = []
        for d in far_first(nz):
            z, peer = z_peer(d)
            out.append(copy(a_src.at[rows(z, nq)], a_dst.at[rows(my_z, nq)], a_ss.at[d], a_rs.at[d], peer))
        return out

    def b_copies():
        out = []
        for d in far_first(nq):
            q, peer = q_peer(d)
            out.append(copy(b_src.at[rows(q, nz)], b_dst.at[rows(my_q, nz)], b_ss.at[d], b_rs.at[d], peer))
        return out

    def spread(planes):
        v = vecs[U]
        for slot, p in enumerate(planes):
            value = x_spline[p, 0:1, :]
            slope = x_spline[p, 1:2, :]
            band = slice(slot * GRID, (slot + 1) * GRID)
            hi, lo = split(y_t[...] * (v[0:1] * slope) + dy_t[...] * (v[1:2] * value))
            lhs_hi[band, :atoms] = hi
            lhs_lo[band, :atoms] = lo
            hi, lo = split(y_t[...] * (v[2:3] * value))
            lhs_hi[band, atoms:] = hi
            lhs_lo[band, atoms:] = lo
        size = len(planes) * GRID
        wide = fast_dot(lhs_hi[:size, :], zz[...])
        return wide[:, :GRID] + wide[:, GRID:] + fast_dot(lhs_lo[:size, :], zz[:, :GRID])

    chunk = 32

    def pair_block(b, carry):
        v_rows, p_rows = [], []
        for e in range(2 * HALO_BLK + 1):
            tile = ext[b + e]
            shift = jnp.where(b + e < HALO_BLK, -1.0 * blocks, jnp.where(b + e >= HALO_BLK + blocks, 1.0 * blocks, 0.0)).astype(F32)
            v_rows.append(tile[0:3] * link[b, e])
            p_rows.append((tile[3:4] + shift, tile[4:5], tile[5:6]))

        def strip(i, inner):
            at_rows = pl.ds(pl.multiple_of(b * TILE + i * chunk, chunk), chunk)
            hx, hy, hz = home[0, at_rows, :], home[1, at_rows, :], home[2, at_rows, :]
            ax = jnp.zeros((chunk, TILE), F32)
            ay, az = ax, ax
            for e in range(2 * HALO_BLK + 1):
                px, py, pz = p_rows[e]
                vx, vy, vz = v_rows[e][0:1], v_rows[e][1:2], v_rows[e][2:3]
                dx, dy, dz = hx - px, hy - py, hz - pz
                inverse = lax.rsqrt(dx * dx + dy * dy + dz * dz + 1.0)
                inverse_sq = inverse * inverse
                third = inverse_sq * inverse
                along = (dx * vx + dy * vy + dz * vz) * (third * inverse_sq) * 3.0
                ax = ax + (third * vx - along * dx)
                ay = ay + (third * vy - along * dy)
                az = az + (third * vz - along * dz)
            pair_acc[0, at_rows, :] = ax
            pair_acc[1, at_rows, :] = ay
            pair_acc[2, at_rows, :] = az
            return inner

        lax.fori_loop(0, TILE // chunk, strip, 0)
        cols = rows(b, TILE)
        for c in range(3):
            near[c : c + 1, cols] = jnp.sum(pair_acc[c, cols, :].T, axis=0, keepdims=True)
        return carry

    arrival = (2,) + tuple(2 - OFFSETS[k] for k in (2, 3, 0, 1))

    def gather(first, last):
        wide = 256
        band = slice(first * GRID, last * GRID)

        def chunk_of(g, carry):
            cols = rows(g, wide)
            tilt_cols = pl.ds(pl.multiple_of(atoms + g * wide, wide), wide)
            plain = fast_dot(pot3[band, :], zt3[:, cols])
            tilted = fast_dot(pot3[band, :], zt3[:, tilt_cols])
            sa = jnp.zeros((GRID, wide), F32)
            sb, sc = sa, sa
            for slot, p in enumerate(arrival[first:last]):
                here = slice(slot * GRID, (slot + 1) * GRID)
                value = x_spline[p, 0:1, cols]
                sa = sa + x_spline[p, 1:2, cols] * plain[here]
                sb = sb + value * plain[here]
                sc = sc + value * tilted[here]
            for c, part in enumerate((sa * y_t[:, cols], sb * dy_t[:, cols], sc * y_t[:, cols])):
                total = jnp.sum(part, axis=0, keepdims=True)
                far[c : c + 1, cols] = total if first == 0 else far[c : c + 1, cols] + total
            return carry

        lax.fori_loop(0, atoms // wide, chunk_of, 0)

    def put_plane(p, plane):
        hi, lo = split(plane)
        at = arrival.index(p)
        band = slice(at * GRID, (at + 1) * GRID)
        pot3[band, :GRID] = hi
        pot3[band, GRID : 2 * GRID] = lo
        pot3[band, 2 * GRID :] = hi

    def put_vector():
        v = vecs[U]
        for b in range(blocks):
            ext[HALO_BLK + b, 0:3, :] = v[:, b * TILE : (b + 1) * TILE]

    def spread_pair(pair):
        both = spread([OFFSETS[k] + 2 for k in pair])
        for slot, k in enumerate(pair):
            rim[k] = both[slot * GRID : (slot + 1) * GRID]

    yz_copy.wait()
    lax.fori_loop(0, blocks, prepare, 0)
    vecs[R] = field[...]
    vecs[U] = field[...] / ip
    for name in (PP, S, X):
        vecs[name] = jnp.zeros((3, atoms), F32)
    scal[...] = jnp.ones_like(scal)
    ra_src[...] = jnp.zeros_like(ra_src)
    put_vector()
    spread_pair((0, 1))
    spread_pair((2, 3))
    own_plane[...] = spread([2])
    lax.fori_loop(0, blocks, prepare_more, 0)
    prepare_green()
    pl.semaphore_wait(barrier, (nz - 1) + (nq - 1) + len(OFFSETS))
    for k in range(len(OFFSETS)):
        rim_copy(k).start()
    for c in vec_copies():
        c.start()

    def sweep(it, carry):
        own = own_plane[...]
        for k in range(len(OFFSETS)):
            rim_copy(k).wait_recv()
            own = own + rim_in[k]
        f1_src[...] = left_dot(fwd_left, right_dot(own, fwd_right))
        for c in f1_copies():
            c.start()
        f1_dst[rows(my_q, nz), :] = f1_src[rows(my_q, nz), :]

        for c in vec_copies():
            c.wait_recv()
        lax.fori_loop(0, 2, pair_block, 0)

        for c in f1_copies():
            c.wait_recv()
        for z in range(nz):
            f2_src[z * nq : (z + 1) * nq, :] = f1_dst[pl.ds(z, nq, stride=nz), :]
        for c in f2_copies():
            c.start()
        f2_dst[rows(my_z, nq), :] = f2_src[rows(my_z, nq), :]

        lax.fori_loop(2, blocks, pair_block, 0)

        for c in f2_copies():
            c.wait_recv()
        lines = left_dot(x_left, f2_dst[...])
        scaled = lines * green[...]
        a_src[...] = left_dot(xt_left, scaled)
        for c in a_copies():
            c.start()
        a_dst[rows(my_z, nq), :] = a_src[rows(my_z, nq), :]
        reduce_start(jnp.sum(lines * scaled, axis=0, keepdims=True))
        for c in a_copies():
            c.wait_recv()
        for q in range(nq):
            b_src[q * nz : (q + 1) * nz, :] = a_dst[pl.ds(q, nz, stride=nq), :]
        for c in b_copies():
            c.start()
        b_dst[rows(my_q, nz), :] = b_src[rows(my_q, nz), :]
        reduce_middle()
        for c in b_copies():
            c.wait_recv()
        mine = right_dot(left_dot(inv_left, b_dst[...]), inv_right)
        pot[...] = mine
        for k in (2, 3, 0, 1):
            pot_copy(k).start()
        put_plane(2, mine)
        for group in (vec_copies(), f1_copies(), f2_copies(), a_copies(), b_copies()):
            for c in group:
                c.wait_send()
        for k in range(len(OFFSETS)):
            rim_copy(k).wait_send()
        for k in (2, 3):
            pot_copy(k).wait_recv()
            put_plane(2 - OFFSETS[k], pot_in[k])
        gather(0, 3)
        for k in (0, 1):
            pot_copy(k).wait_recv()
            put_plane(2 - OFFSETS[k], pot_in[k])
        gather(3, ORDER)
        u = vecs[U]
        image = ip * u + far[...] - PAIR_C * (near[...] - u)
        gamma, delta = reduce_end()
        beta = jnp.where(it == 0, 0.0, gamma / scal[0, 0:1, 0:1])
        alpha = gamma / (delta - beta * gamma / scal[1, 0:1, 0:1])
        scal[0] = jnp.broadcast_to(gamma, (8, TILE))
        scal[1] = jnp.broadcast_to(alpha, (8, TILE))
        new_p = u + beta * vecs[PP]
        new_s = image + beta * vecs[S]
        vecs[PP] = new_p
        vecs[S] = new_s

        @pl.when(it < ITERS - 1)
        def _():
            residual = vecs[R] - alpha * new_s
            vecs[U] = residual / ip
            put_vector()
            for c in vec_copies():
                c.start()
            vecs[R] = residual
            vecs[X] = vecs[X] + alpha * new_p
            for pair in ((0, 1), (2, 3)):
                spread_pair(pair)
                for k in pair:
                    rim_copy(k).start()
            own_plane[...] = spread([2])

        @pl.when(it == ITERS - 1)
        def _():
            dip_a[...] = vecs[X]
            dip_b[...] = new_p
            step_out[...] = jnp.broadcast_to(alpha, (3, atoms))
            res_a[...] = vecs[R]
            res_b[...] = new_s

        for k in range(len(OFFSETS)):
            pot_copy(k).wait_send()
        return carry

    lax.fori_loop(0, ITERS, sweep, 0)


def per_device(n, positions, field, inv_polar, x_spline, yz_spline, tile_list, tile_count):
    atoms = positions.shape[1]
    blocks = atoms // TILE
    nq = NX * NC
    nz = n // nq
    rows_x = np.arange(GRID)
    q, z = rows_x % nq, rows_x // nq
    plane = (q // NC) * (nz * NC) + z * NC + q % NC
    table = basis(GRID)
    across = table[:, plane]

    def parts(t):
        whole = jnp.asarray(t, F32)
        return split(whole)

    def left_of(t):
        hi, lo = parts(t)
        return jnp.concatenate([hi, lo, hi], axis=1)

    def right_of(t):
        hi, lo = parts(t)
        return jnp.concatenate([hi, hi, lo], axis=0)

    with jax.ensure_compile_time_eval():
        tables = (right_of(table.T), left_of(table), left_of(across), left_of(across.T), left_of(table.T), right_of(table))
    vm = pl.BlockSpec(memory_space=pltpu.VMEM)
    sm = pl.BlockSpec(memory_space=pltpu.SMEM)
    square = pltpu.VMEM((GRID, GRID), F32)
    sem = pltpu.SemaphoreType.DMA
    out = jax.ShapeDtypeStruct((3, atoms), F32)
    dip_a, dip_b, res_a, res_b, step = pl.pallas_call(
        functools.partial(solve_kernel, n),
        out_shape=(out,) * 5,
        in_specs=[sm, sm] + [vm] * 4 + [pl.BlockSpec(memory_space=pl.ANY)] + [vm] * 6,
        out_specs=(vm,) * 5,
        scratch_shapes=[
            pltpu.VMEM(yz_spline.shape, F32),
            sem,
            pltpu.SMEM((blocks, 2 * HALO_BLK + 1), F32),
            pltpu.VMEM((blocks + 2 * HALO_BLK, 8, TILE), F32),
            pltpu.VMEM((3, atoms, TILE), F32),
            pltpu.VMEM((3, atoms, TILE), F32),
            pltpu.VMEM((3, atoms), F32),
            pltpu.VMEM((3, atoms), F32),
            pltpu.VMEM((GRID, atoms), F32),
            pltpu.VMEM((GRID, atoms), F32),
            pltpu.VMEM((2 * atoms, 2 * GRID), BF16),
            pltpu.VMEM((3 * GRID, 2 * atoms), BF16),
            pltpu.VMEM((2 * GRID, 2 * atoms), BF16),
            pltpu.VMEM((2 * GRID, 2 * atoms), BF16),
            pltpu.VMEM((4, GRID, GRID), F32),
            pltpu.VMEM((4, GRID, GRID), F32),
            square,
            square,
            pltpu.VMEM((4, GRID, GRID), F32),
            pltpu.VMEM((ORDER * GRID, 3 * GRID), BF16),
            square,
            square, square, square, square,
            square, square, square, square,
            pltpu.VMEM((8, TILE), F32),
            pltpu.VMEM((nz, 8, TILE), F32),
            pltpu.VMEM((8, TILE), F32),
            pltpu.VMEM((nq, 8, TILE), F32),
            pltpu.VMEM((5, 3, atoms), F32),
            pltpu.VMEM((2, 8, TILE), F32),
            sem((2,)), sem((2,)),
            sem((4,)), sem((4,)),
            sem((4,)), sem((4,)),
            sem((nq,)), sem((nq,)),
            sem((nz,)), sem((nz,)),
            sem((nz,)), sem((nz,)),
            sem((nq,)), sem((nq,)),
            sem((nz,)), sem((nz,)),
            sem((nq,)), sem((nq,)),
        ],
        compiler_params=pltpu.CompilerParams(
            collective_id=0, has_side_effects=True, vmem_limit_bytes=56 * 1024 * 1024
        ),
    )(tile_list, tile_count, positions, field, inv_polar.reshape(1, atoms), x_spline.transpose(1, 0, 2), yz_spline,
      *tables)
    return dip_a + step * dip_b, res_a - step * res_b


def solution(mesh):
    both = ("rep", "gx")
    in_specs = (
        P(None, both),
        P(None, both),
        P(both),
        P(None, None, both),
        P(None, both, None),
        P(both, None),
        P(both),
    )
    out_specs = (P(None, both), P(None, both))
    return jax.shard_map(
        functools.partial(per_device, mesh.shape["gx"]),
        mesh=mesh, in_specs=in_specs, out_specs=out_specs, check_vma=False,
    )
```

```python
import functools

import jax
import jax.numpy as jnp
import numpy as np
from jax import lax
from jax.experimental import pallas as pl
from jax.experimental.pallas import tpu as pltpu
from jax.sharding import PartitionSpec as P

GRID = 128
ORDER = 5
TILE = 128
HALO_BLK = 3
ITERS = 3
PAIR_C = 0.025
RECIP_C = 8192.0
DAMP = 0.0008
MESH = pl.DeviceIdType.MESH
F32 = jnp.float32
BF16 = jnp.bfloat16
NX = 4
NC = 2
OFFSETS = (-2, 2, -1, 1)


def far_first(count):
    return sorted(range(1, count), key=lambda d: -min(d, count - d))


def basis(size):
    freq = np.arange(size)
    half = size // 2
    mode = np.where(freq <= half, freq, freq - half)
    angle = (mode[:, None] * np.arange(size)[None, :] % size) * (2.0 * np.pi / size)
    return np.where((freq <= half)[:, None], np.cos(angle), np.sin(angle))


def split(x):
    hi = x.astype(BF16)
    return hi, (x - hi.astype(F32)).astype(BF16)


def left_dot(stacked, x):
    hi, lo = split(x)
    return fast_dot(stacked[...], jnp.concatenate([hi, hi, lo], axis=0))


def right_dot(x, stacked):
    hi, lo = split(x)
    return fast_dot(jnp.concatenate([hi, lo, hi], axis=1), stacked[...])


def fast_dot(a, b):
    return jnp.dot(a, b, preferred_element_type=F32)


def mode_of(freq, size):
    half = size // 2
    mode = jnp.where(freq <= half, freq, freq - half)
    weight = jnp.where((freq == 0) | (freq == half), 1.0 / size, 2.0 / size)
    return mode.astype(F32), weight.astype(F32)


def solve_kernel(
    n,
    tile_list,
    tile_count,
    pos,
    field,
    inv_polar,
    x_spline,
    yz_hbm,
    fwd_right,
    fwd_left,
    inv_left,
    inv_right,
    dip_a,
    dip_b,
    res_a,
    res_b,
    step_out,
    yz,
    yz_sem,
    link,
    ext,
    home,
    pair_acc,
    near,
    far,
    y_t,
    dy_t,
    zz,
    zt3,
    lhs_hi,
    lhs_lo,
    rim,
    rim_in,
    own_plane,
    pot,
    pot_in,
    pot3,
    green,
    f_src,
    f_dst,
    a_src,
    a_dst,
    ra_src,
    ra_dst,
    rb_src,
    rb_dst,
    vecs,
    scal,
    v_ss,
    v_rs,
    c_ss,
    c_rs,
    h_ss,
    h_rs,
    f_ss,
    f_rs,
    a_ss,
    a_rs,
    ra_ss,
    ra_rs,
    rb_ss,
    rb_rs,
):
    nq = NX * NC
    nz = n // nq
    me = lax.axis_index("gx")
    my_q = (me // (nz * NC)) * NC + me % NC
    my_z = me % (nz * NC) // NC
    blocks = pos.shape[1] // TILE
    atoms = pos.shape[1]

    def at(q, z):
        return (q // NC) * (nz * NC) + z * NC + q % NC

    def q_peer(d):
        q = (my_q + d) % nq
        return q, at(q, my_z)

    def z_peer(d):
        z = (my_z + d) % nz
        return z, at(my_q, z)

    def to(d):
        return (me + d + n) % n

    def copy(src, dst, ss, rs, peer):
        return pltpu.make_async_remote_copy(
            src_ref=src, dst_ref=dst, send_sem=ss, recv_sem=rs,
            device_id={"gx": peer}, device_id_type=MESH,
        )

    def rows(i, size):
        return pl.ds(pl.multiple_of(i * size, size), size)

    yz_copy = pltpu.make_async_copy(yz_hbm, yz, yz_sem)
    yz_copy.start()

    barrier = pltpu.get_barrier_semaphore()
    def greet(peer):
        pl.semaphore_signal(barrier, inc=1, device_id={"gx": peer}, device_id_type=MESH)

    def every_peer(visit):
        def ring(i, carry):
            half = (i + 1) // 2
            z = (my_z + nz // 2 + jnp.where(i % 2 == 1, -half, half) + nz) % nz
            for d in range(nq):
                visit(at((my_q + d) % nq, z))
            return carry

        lax.fori_loop(0, nz - 1, ring, 0)
        for d in far_first(nq):
            visit(q_peer(d)[1])

    every_peer(greet)

    def prepare(b, carry):
        cols = rows(b, TILE)
        y_t[:, cols] = yz[0, cols, :].T
        dy_t[:, cols] = yz[1, cols, :].T
        for part in range(2):
            hi, lo = split(yz[2 + part, cols, :])
            at_rows = pl.ds(pl.multiple_of(part * atoms + b * TILE, TILE), TILE)
            zz[at_rows, :GRID] = hi
            zz[at_rows, GRID:] = lo
        ext[HALO_BLK + b, 3:6, :] = pos[:, cols]
        return carry

    def prepare_more(b, carry):
        cols = rows(b, TILE)
        for part in range(2):
            at_rows = pl.ds(pl.multiple_of(part * atoms + b * TILE, TILE), TILE)
            hi, lo = split(yz[2 + part, cols, :].T)
            zt3[:GRID, at_rows] = hi
            zt3[GRID : 2 * GRID, at_rows] = hi
            zt3[2 * GRID :, at_rows] = lo
        here = pos[:, cols]
        for c in range(3):
            home[c, cols, :] = jnp.broadcast_to(here[c : c + 1], (TILE, TILE)).T
        for e in range(2 * HALO_BLK + 1):
            total = jnp.float32(0.0)
            for k in range(tile_list.shape[1]):
                hit = (tile_list[b, k] == b + e) & (k < tile_count[b])
                total = total + jnp.where(hit, jnp.float32(1.0), jnp.float32(0.0))
            link[b, e] = total
        return carry

    def prepare_green():
        row_freq = lax.broadcasted_iota(jnp.int32, (GRID, GRID), 0)
        col_freq = lax.broadcasted_iota(jnp.int32, (GRID, GRID), 1)
        kx, wx = mode_of(row_freq, GRID)
        kz, wz = mode_of(col_freq, GRID)
        ky, wy = mode_of(jnp.full((GRID, GRID), me, jnp.int32), GRID)
        mode_sq = kx * kx + ky * ky + kz * kz
        safe_sq = jnp.where(mode_sq > 0, mode_sq, 1.0)
        green[...] = jnp.where(mode_sq > 0, RECIP_C * jnp.exp(-DAMP * safe_sq) / safe_sq, 0.0) * wx * wy * wz

    ip = inv_polar[...]
    R, U, PP, S, X = range(5)

    def reduce_a():
        return [copy(ra_src, ra_dst.at[my_z], ra_ss.at[d], ra_rs.at[d], z_peer(d)[1]) for d in far_first(nz)]

    def reduce_b():
        return [copy(rb_src, rb_dst.at[my_q], rb_ss.at[d], rb_rs.at[d], q_peer(d)[1]) for d in far_first(nq)]

    def folded(value):
        lanes = sum(value[:, k * TILE : (k + 1) * TILE] for k in range(atoms // TILE))
        return jnp.sum(lanes, axis=0, keepdims=True)

    def reduce_start(energy):
        u = vecs[U]
        ra_src[0:1, :] = folded(vecs[R] * u)
        ra_src[1:2, :] = folded((ip * u - PAIR_C * (near[...] - u)) * u) + energy
        ra_dst[my_z] = ra_src[...]
        for c in reduce_a():
            c.start()

    def reduce_middle():
        for c in reduce_a():
            c.wait_recv()
        rb_src[...] = jnp.sum(ra_dst[...], axis=0)
        rb_dst[my_q] = rb_src[...]
        for c in reduce_b():
            c.start()

    def reduce_end():
        for c in reduce_b():
            c.wait_recv()
        sums = jnp.sum(jnp.sum(rb_dst[...], axis=0), axis=1, keepdims=True)
        for c in reduce_a():
            c.wait_send()
        for c in reduce_b():
            c.wait_send()
        return sums[0:1], sums[1:2]

    def vec_copies():
        return [
            copy(ext.at[pl.ds(HALO_BLK, HALO_BLK)], ext.at[pl.ds(HALO_BLK + blocks, HALO_BLK)], v_ss.at[0], v_rs.at[0], to(-1)),
            copy(ext.at[pl.ds(blocks, HALO_BLK)], ext.at[pl.ds(0, HALO_BLK)], v_ss.at[1], v_rs.at[1], to(1)),
        ]

    def rim_copy(k):
        return copy(rim.at[k], rim_in.at[k], c_ss.at[k], c_rs.at[k], to(OFFSETS[k]))

    def pot_copy(k):
        return copy(pot, pot_in.at[k], h_ss.at[k], h_rs.at[k], to(OFFSETS[k]))

    def row(i):
        return pl.ds(i, 1)

    def exchange_start(src, dst, ss, rs):
        every_peer(lambda peer: copy(src.at[row(peer)], dst.at[row(me)], ss, rs, peer).start())
        dst[row(me), :] = src[row(me), :]

    def exchange_all(src, dst, ss, rs):
        return copy(src.at[pl.ds(0, n - 1)], dst.at[pl.ds(0, n - 1)], ss, rs, to(1))

    def spread(planes):
        v = vecs[U]
        for slot, p in enumerate(planes):
            value = x_spline[p, 0:1, :]
            slope = x_spline[p, 1:2, :]
            band = slice(slot * GRID, (slot + 1) * GRID)
            hi, lo = split(y_t[...] * (v[0:1] * slope) + dy_t[...] * (v[1:2] * value))
            lhs_hi[band, :atoms] = hi
            lhs_lo[band, :atoms] = lo
            hi, lo = split(y_t[...] * (v[2:3] * value))
            lhs_hi[band, atoms:] = hi
            lhs_lo[band, atoms:] = lo
        size = len(planes) * GRID
        wide = fast_dot(lhs_hi[:size, :], zz[...])
        return wide[:, :GRID] + wide[:, GRID:] + fast_dot(lhs_lo[:size, :], zz[:, :GRID])

    chunk = 32

    def pair_block(b, carry):
        v_rows, p_rows = [], []
        for e in range(2 * HALO_BLK + 1):
            tile = ext[b + e]
            shift = jnp.where(b + e < HALO_BLK, -1.0 * blocks, jnp.where(b + e >= HALO_BLK + blocks, 1.0 * blocks, 0.0)).astype(F32)
            v_rows.append(tile[0:3] * link[b, e])
            p_rows.append((tile[3:4] + shift, tile[4:5], tile[5:6]))

        def strip(i, inner):
            at_rows = pl.ds(pl.multiple_of(b * TILE + i * chunk, chunk), chunk)
            hx, hy, hz = home[0, at_rows, :], home[1, at_rows, :], home[2, at_rows, :]
            ax = jnp.zeros((chunk, TILE), F32)
            ay, az = ax, ax
            for e in range(2 * HALO_BLK + 1):
                px, py, pz = p_rows[e]
                vx, vy, vz = v_rows[e][0:1], v_rows[e][1:2], v_rows[e][2:3]
                dx, dy, dz = hx - px, hy - py, hz - pz
                inverse = lax.rsqrt(dx * dx + dy * dy + dz * dz + 1.0)
                inverse_sq = inverse * inverse
                third = inverse_sq * inverse
                along = (dx * vx + dy * vy + dz * vz) * (third * inverse_sq) * 3.0
                ax = ax + (third * vx - along * dx)
                ay = ay + (third * vy - along * dy)
                az = az + (third * vz - along * dz)
            pair_acc[0, at_rows, :] = ax
            pair_acc[1, at_rows, :] = ay
            pair_acc[2, at_rows, :] = az
            return inner

        lax.fori_loop(0, TILE // chunk, strip, 0)
        cols = rows(b, TILE)
        for c in range(3):
            near[c : c + 1, cols] = jnp.sum(pair_acc[c, cols, :].T, axis=0, keepdims=True)
        return carry

    arrival = (2,) + tuple(2 - OFFSETS[k] for k in (2, 3, 0, 1))

    def gather(first, last):
        wide = 256
        band = slice(first * GRID, last * GRID)

        def chunk_of(g, carry):
            cols = rows(g, wide)
            tilt_cols = pl.ds(pl.multiple_of(atoms + g * wide, wide), wide)
            plain = fast_dot(pot3[band, :], zt3[:, cols])
            tilted = fast_dot(pot3[band, :], zt3[:, tilt_cols])
            sa = jnp.zeros((GRID, wide), F32)
            sb, sc = sa, sa
            for slot, p in enumerate(arrival[first:last]):
                here = slice(slot * GRID, (slot + 1) * GRID)
                value = x_spline[p, 0:1, cols]
                sa = sa + x_spline[p, 1:2, cols] * plain[here]
                sb = sb + value * plain[here]
                sc = sc + value * tilted[here]
            for c, part in enumerate((sa * y_t[:, cols], sb * dy_t[:, cols], sc * y_t[:, cols])):
                total = jnp.sum(part, axis=0, keepdims=True)
                far[c : c + 1, cols] = total if first == 0 else far[c : c + 1, cols] + total
            return carry

        lax.fori_loop(0, atoms // wide, chunk_of, 0)

    def put_plane(p, plane):
        hi, lo = split(plane)
        at = arrival.index(p)
        band = slice(at * GRID, (at + 1) * GRID)
        pot3[band, :GRID] = hi
        pot3[band, GRID : 2 * GRID] = lo
        pot3[band, 2 * GRID :] = hi

    def put_vector():
        v = vecs[U]
        for b in range(blocks):
            ext[HALO_BLK + b, 0:3, :] = v[:, b * TILE : (b + 1) * TILE]

    def spread_pair(pair):
        both = spread([OFFSETS[k] + 2 for k in pair])
        for slot, k in enumerate(pair):
            rim[k] = both[slot * GRID : (slot + 1) * GRID]

    yz_copy.wait()
    lax.fori_loop(0, blocks, prepare, 0)
    vecs[R] = field[...]
    vecs[U] = field[...] / ip
    for name in (PP, S, X):
        vecs[name] = jnp.zeros((3, atoms), F32)
    scal[...] = jnp.ones_like(scal)
    ra_src[...] = jnp.zeros_like(ra_src)
    put_vector()
    spread_pair((0, 1))
    spread_pair((2, 3))
    own_plane[...] = spread([2])
    lax.fori_loop(0, blocks, prepare_more, 0)
    prepare_green()
    pl.semaphore_wait(barrier, n - 1)
    for k in range(len(OFFSETS)):
        rim_copy(k).start()
    for c in vec_copies():
        c.start()

    def sweep(it, carry):
        own = own_plane[...]
        for k in range(len(OFFSETS)):
            rim_copy(k).wait_recv()
            own = own + rim_in[k]
        f_src[...] = left_dot(fwd_left, right_dot(own, fwd_right))
        exchange_start(f_src, f_dst, f_ss, f_rs)

        for c in vec_copies():
            c.wait_recv()
        lax.fori_loop(0, blocks, pair_block, 0)

        exchange_all(f_src, f_dst, f_ss, f_rs).wait_recv()
        lines = left_dot(fwd_left, f_dst[...])
        scaled = lines * green[...]
        a_src[...] = left_dot(inv_left, scaled)
        exchange_start(a_src, a_dst, a_ss, a_rs)
        reduce_start(jnp.sum(lines * scaled, axis=0, keepdims=True))
        exchange_all(a_src, a_dst, a_ss, a_rs).wait_recv()
        reduce_middle()
        mine = right_dot(left_dot(inv_left, a_dst[...]), inv_right)
        pot[...] = mine
        for k in (2, 3, 0, 1):
            pot_copy(k).start()
        put_plane(2, mine)
        for c in vec_copies():
            c.wait_send()
        exchange_all(f_src, f_dst, f_ss, f_rs).wait_send()
        exchange_all(a_src, a_dst, a_ss, a_rs).wait_send()
        for k in range(len(OFFSETS)):
            rim_copy(k).wait_send()
        for k in (2, 3):
            pot_copy(k).wait_recv()
            put_plane(2 - OFFSETS[k], pot_in[k])
        gather(0, 3)
        for k in (0, 1):
            pot_copy(k).wait_recv()
            put_plane(2 - OFFSETS[k], pot_in[k])
        gather(3, ORDER)
        u = vecs[U]
        image = ip * u + far[...] - PAIR_C * (near[...] - u)
        gamma, delta = reduce_end()
        beta = jnp.where(it == 0, 0.0, gamma / scal[0, 0:1, 0:1])
        alpha = gamma / (delta - beta * gamma / scal[1, 0:1, 0:1])
        scal[0] = jnp.broadcast_to(gamma, (8, TILE))
        scal[1] = jnp.broadcast_to(alpha, (8, TILE))
        new_p = u + beta * vecs[PP]
        new_s = image + beta * vecs[S]
        vecs[PP] = new_p
        vecs[S] = new_s

        @pl.when(it < ITERS - 1)
        def _():
            residual = vecs[R] - alpha * new_s
            vecs[U] = residual / ip
            put_vector()
            for c in vec_copies():
                c.start()
            vecs[R] = residual
            vecs[X] = vecs[X] + alpha * new_p
            for pair in ((0, 1), (2, 3)):
                spread_pair(pair)
                for k in pair:
                    rim_copy(k).start()
            own_plane[...] = spread([2])

        @pl.when(it == ITERS - 1)
        def _():
            dip_a[...] = vecs[X]
            dip_b[...] = new_p
            step_out[...] = jnp.broadcast_to(alpha, (3, atoms))
            res_a[...] = vecs[R]
            res_b[...] = new_s

        for k in range(len(OFFSETS)):
            pot_copy(k).wait_send()
        return carry

    lax.fori_loop(0, ITERS, sweep, 0)


def per_device(n, positions, field, inv_polar, x_spline, yz_spline, tile_list, tile_count):
    atoms = positions.shape[1]
    blocks = atoms // TILE
    nq = NX * NC
    nz = n // nq
    table = basis(GRID)

    def parts(t):
        whole = jnp.asarray(t, F32)
        return split(whole)

    def left_of(t):
        hi, lo = parts(t)
        return jnp.concatenate([hi, lo, hi], axis=1)

    def right_of(t):
        hi, lo = parts(t)
        return jnp.concatenate([hi, hi, lo], axis=0)

    with jax.ensure_compile_time_eval():
        tables = (right_of(table.T), left_of(table), left_of(table.T), right_of(table))
    vm = pl.BlockSpec(memory_space=pltpu.VMEM)
    sm = pl.BlockSpec(memory_space=pltpu.SMEM)
    square = pltpu.VMEM((GRID, GRID), F32)
    sem = pltpu.SemaphoreType.DMA
    out = jax.ShapeDtypeStruct((3, atoms), F32)
    dip_a, dip_b, res_a, res_b, step = pl.pallas_call(
        functools.partial(solve_kernel, n),
        out_shape=(out,) * 5,
        in_specs=[sm, sm] + [vm] * 4 + [pl.BlockSpec(memory_space=pl.ANY)] + [vm] * 4,
        out_specs=(vm,) * 5,
        scratch_shapes=[
            pltpu.VMEM(yz_spline.shape, F32),
            sem,
            pltpu.SMEM((blocks, 2 * HALO_BLK + 1), F32),
            pltpu.VMEM((blocks + 2 * HALO_BLK, 8, TILE), F32),
            pltpu.VMEM((3, atoms, TILE), F32),
            pltpu.VMEM((3, atoms, TILE), F32),
            pltpu.VMEM((3, atoms), F32),
            pltpu.VMEM((3, atoms), F32),
            pltpu.VMEM((GRID, atoms), F32),
            pltpu.VMEM((GRID, atoms), F32),
            pltpu.VMEM((2 * atoms, 2 * GRID), BF16),
            pltpu.VMEM((3 * GRID, 2 * atoms), BF16),
            pltpu.VMEM((2 * GRID, 2 * atoms), BF16),
            pltpu.VMEM((2 * GRID, 2 * atoms), BF16),
            pltpu.VMEM((4, GRID, GRID), F32),
            pltpu.VMEM((4, GRID, GRID), F32),
            square,
            square,
            pltpu.VMEM((4, GRID, GRID), F32),
            pltpu.VMEM((ORDER * GRID, 3 * GRID), BF16),
            square,
            square, square, square, square,
            pltpu.VMEM((8, TILE), F32),
            pltpu.VMEM((nz, 8, TILE), F32),
            pltpu.VMEM((8, TILE), F32),
            pltpu.VMEM((nq, 8, TILE), F32),
            pltpu.VMEM((5, 3, atoms), F32),
            pltpu.VMEM((2, 8, TILE), F32),
            sem((2,)), sem((2,)),
            sem((4,)), sem((4,)),
            sem((4,)), sem((4,)),
            sem, sem, sem, sem,
            sem((nz,)), sem((nz,)),
            sem((nq,)), sem((nq,)),
        ],
        compiler_params=pltpu.CompilerParams(
            collective_id=0, has_side_effects=True, vmem_limit_bytes=56 * 1024 * 1024
        ),
    )(tile_list, tile_count, positions, field, inv_polar.reshape(1, atoms), x_spline.transpose(1, 0, 2), yz_spline,
      *tables)
    return dip_a + step * dip_b, res_a - step * res_b


def solution(mesh):
    both = ("rep", "gx")
    in_specs = (
        P(None, both),
        P(None, both),
        P(both),
        P(None, None, both),
        P(None, both, None),
        P(both, None),
        P(both),
    )
    out_specs = (P(None, both), P(None, both))
    return jax.shard_map(
        functools.partial(per_device, mesh.shape["gx"]),
        mesh=mesh, in_specs=in_specs, out_specs=out_specs, check_vma=False,
    )
```

```python
import functools

import jax
import jax.numpy as jnp
import numpy as np
from jax import lax
from jax.experimental import pallas as pl
from jax.experimental.pallas import tpu as pltpu
from jax.sharding import PartitionSpec as P

GRID = 128
ORDER = 5
TILE = 128
HALO_BLK = 3
ITERS = 3
PAIR_C = 0.025
RECIP_C = 8192.0
DAMP = 0.0008
MESH = pl.DeviceIdType.MESH
F32 = jnp.float32
BF16 = jnp.bfloat16
NX = 4
NC = 2
OFFSETS = (-2, 2, -1, 1)


def far_first(count):
    return sorted(range(1, count), key=lambda d: -min(d, count - d))


def basis(size):
    freq = np.arange(size)
    half = size // 2
    mode = np.where(freq <= half, freq, freq - half)
    angle = (mode[:, None] * np.arange(size)[None, :] % size) * (2.0 * np.pi / size)
    return np.where((freq <= half)[:, None], np.cos(angle), np.sin(angle))


def split(x):
    hi = x.astype(BF16)
    return hi, (x - hi.astype(F32)).astype(BF16)


def left_dot(stacked, x):
    hi, lo = split(x)
    return fast_dot(stacked[...], jnp.concatenate([hi, hi, lo], axis=0))


def right_dot(x, stacked):
    hi, lo = split(x)
    return fast_dot(jnp.concatenate([hi, lo, hi], axis=1), stacked[...])


def fast_dot(a, b):
    return jnp.dot(a, b, preferred_element_type=F32)


def mode_of(freq, size):
    half = size // 2
    mode = jnp.where(freq <= half, freq, freq - half)
    weight = jnp.where((freq == 0) | (freq == half), 1.0 / size, 2.0 / size)
    return mode.astype(F32), weight.astype(F32)


def solve_kernel(
    n,
    tile_list,
    tile_count,
    pos,
    field,
    inv_polar,
    x_spline,
    yz_hbm,
    fwd_right,
    fwd_left,
    inv_left,
    inv_right,
    dip_a,
    dip_b,
    res_a,
    res_b,
    step_out,
    yz,
    yz_sem,
    link,
    ext,
    home,
    pair_acc,
    near,
    far,
    y_t,
    dy_t,
    zz,
    zt3,
    lhs_hi,
    lhs_lo,
    rim,
    rim_in,
    own_plane,
    pot,
    pot_in,
    pot3,
    green,
    f_src,
    f_dst,
    a_src,
    a_dst,
    ra_src,
    ra_dst,
    rb_src,
    rb_dst,
    vecs,
    scal,
    v_ss,
    v_rs,
    c_ss,
    c_rs,
    h_ss,
    h_rs,
    f_ss,
    f_rs,
    a_ss,
    a_rs,
    ra_ss,
    ra_rs,
    rb_ss,
    rb_rs,
):
    nq = NX * NC
    nz = n // nq
    me = lax.axis_index("gx")
    my_q = (me // (nz * NC)) * NC + me % NC
    my_z = me % (nz * NC) // NC
    blocks = pos.shape[1] // TILE
    atoms = pos.shape[1]

    def at(q, z):
        return (q // NC) * (nz * NC) + z * NC + q % NC

    def q_peer(d):
        q = (my_q + d) % nq
        return q, at(q, my_z)

    def z_peer(d):
        z = (my_z + d) % nz
        return z, at(my_q, z)

    def to(d):
        return (me + d + n) % n

    def copy(src, dst, ss, rs, peer):
        return pltpu.make_async_remote_copy(
            src_ref=src, dst_ref=dst, send_sem=ss, recv_sem=rs,
            device_id={"gx": peer}, device_id_type=MESH,
        )

    def rows(i, size):
        return pl.ds(pl.multiple_of(i * size, size), size)

    yz_copy = pltpu.make_async_copy(yz_hbm, yz, yz_sem)
    yz_copy.start()

    barrier = pltpu.get_barrier_semaphore()
    def greet(peer):
        pl.semaphore_signal(barrier, inc=1, device_id={"gx": peer}, device_id_type=MESH)

    def every_peer(visit):
        def ring(i, carry):
            half = (i + 1) // 2
            z = (my_z + nz // 2 + jnp.where(i % 2 == 1, -half, half) + nz) % nz
            for d in far_first(nq) + [0]:
                visit(at((my_q + d) % nq, z))
            return carry

        lax.fori_loop(0, nz - 1, ring, 0)
        for d in far_first(nq):
            visit(q_peer(d)[1])

    every_peer(greet)

    def prepare(b, carry):
        cols = rows(b, TILE)
        y_t[:, cols] = yz[0, cols, :].T
        dy_t[:, cols] = yz[1, cols, :].T
        for part in range(2):
            hi, lo = split(yz[2 + part, cols, :])
            at_rows = pl.ds(pl.multiple_of(part * atoms + b * TILE, TILE), TILE)
            zz[at_rows, :GRID] = hi
            zz[at_rows, GRID:] = lo
        ext[HALO_BLK + b, 3:6, :] = pos[:, cols]
        return carry

    def prepare_more(b, carry):
        cols = rows(b, TILE)
        for part in range(2):
            at_rows = pl.ds(pl.multiple_of(part * atoms + b * TILE, TILE), TILE)
            hi, lo = split(yz[2 + part, cols, :].T)
            zt3[:GRID, at_rows] = hi
            zt3[GRID : 2 * GRID, at_rows] = hi
            zt3[2 * GRID :, at_rows] = lo
        here = pos[:, cols]
        for c in range(3):
            home[c, cols, :] = jnp.broadcast_to(here[c : c + 1], (TILE, TILE)).T
        for e in range(2 * HALO_BLK + 1):
            total = jnp.float32(0.0)
            for k in range(tile_list.shape[1]):
                hit = (tile_list[b, k] == b + e) & (k < tile_count[b])
                total = total + jnp.where(hit, jnp.float32(1.0), jnp.float32(0.0))
            link[b, e] = total
        return carry

    def prepare_green():
        row_freq = lax.broadcasted_iota(jnp.int32, (GRID, GRID), 0)
        col_freq = lax.broadcasted_iota(jnp.int32, (GRID, GRID), 1)
        kx, wx = mode_of(row_freq, GRID)
        kz, wz = mode_of(col_freq, GRID)
        ky, wy = mode_of(jnp.full((GRID, GRID), me, jnp.int32), GRID)
        mode_sq = kx * kx + ky * ky + kz * kz
        safe_sq = jnp.where(mode_sq > 0, mode_sq, 1.0)
        green[...] = jnp.where(mode_sq > 0, RECIP_C * jnp.exp(-DAMP * safe_sq) / safe_sq, 0.0) * wx * wy * wz

    ip = inv_polar[...]
    R, U, PP, S, X = range(5)

    def reduce_a():
        return [copy(ra_src, ra_dst.at[my_z], ra_ss.at[d], ra_rs.at[d], z_peer(d)[1]) for d in far_first(nz)]

    def reduce_b():
        return [copy(rb_src, rb_dst.at[my_q], rb_ss.at[d], rb_rs.at[d], q_peer(d)[1]) for d in far_first(nq)]

    def folded(value):
        lanes = sum(value[:, k * TILE : (k + 1) * TILE] for k in range(atoms // TILE))
        return jnp.sum(lanes, axis=0, keepdims=True)

    def reduce_start(energy):
        u = vecs[U]
        ra_src[0:1, :] = folded(vecs[R] * u)
        ra_src[1:2, :] = folded((ip * u - PAIR_C * (near[...] - u)) * u) + energy
        ra_dst[my_z] = ra_src[...]
        for c in reduce_a():
            c.start()

    def reduce_middle():
        for c in reduce_a():
            c.wait_recv()
        rb_src[...] = jnp.sum(ra_dst[...], axis=0)
        rb_dst[my_q] = rb_src[...]
        for c in reduce_b():
            c.start()

    def reduce_end():
        for c in reduce_b():
            c.wait_recv()
        sums = jnp.sum(jnp.sum(rb_dst[...], axis=0), axis=1, keepdims=True)
        for c in reduce_a():
            c.wait_send()
        for c in reduce_b():
            c.wait_send()
        return sums[0:1], sums[1:2]

    def vec_copies():
        return [
            copy(ext.at[pl.ds(HALO_BLK, HALO_BLK)], ext.at[pl.ds(HALO_BLK + blocks, HALO_BLK)], v_ss.at[0], v_rs.at[0], to(-1)),
            copy(ext.at[pl.ds(blocks, HALO_BLK)], ext.at[pl.ds(0, HALO_BLK)], v_ss.at[1], v_rs.at[1], to(1)),
        ]

    def rim_copy(k):
        return copy(rim.at[k], rim_in.at[k], c_ss.at[k], c_rs.at[k], to(OFFSETS[k]))

    def pot_copy(k):
        return copy(pot, pot_in.at[k], h_ss.at[k], h_rs.at[k], to(OFFSETS[k]))

    def row(i):
        return pl.ds(i, 1)

    def exchange_start(src, dst, ss, rs):
        every_peer(lambda peer: copy(src.at[row(peer)], dst.at[row(me)], ss, rs, peer).start())
        dst[row(me), :] = src[row(me), :]

    def exchange_all(src, dst, ss, rs):
        return copy(src.at[pl.ds(0, n - 1)], dst.at[pl.ds(0, n - 1)], ss, rs, to(1))

    def spread(p, slot):
        v = vecs[U]
        value = x_spline[p, 0:1, :]
        slope = x_spline[p, 1:2, :]
        band = slice(slot * GRID, (slot + 1) * GRID)
        hi, lo = split(y_t[...] * (v[0:1] * slope) + dy_t[...] * (v[1:2] * value))
        lhs_hi[band, :atoms] = hi
        lhs_lo[band, :atoms] = lo
        hi, lo = split(y_t[...] * (v[2:3] * value))
        lhs_hi[band, atoms:] = hi
        lhs_lo[band, atoms:] = lo
        wide = fast_dot(lhs_hi[band, :], zz[...])
        return wide[:, :GRID] + wide[:, GRID:] + fast_dot(lhs_lo[band, :], zz[:, :GRID])

    chunk = 32

    def pair_block(b, carry):
        v_rows, p_rows = [], []
        for e in range(2 * HALO_BLK + 1):
            tile = ext[b + e]
            shift = jnp.where(b + e < HALO_BLK, -1.0 * blocks, jnp.where(b + e >= HALO_BLK + blocks, 1.0 * blocks, 0.0)).astype(F32)
            v_rows.append(tile[0:3] * link[b, e])
            p_rows.append((tile[3:4] + shift, tile[4:5], tile[5:6]))

        def strip(i, inner):
            at_rows = pl.ds(pl.multiple_of(b * TILE + i * chunk, chunk), chunk)
            hx, hy, hz = home[0, at_rows, :], home[1, at_rows, :], home[2, at_rows, :]
            ax = jnp.zeros((chunk, TILE), F32)
            ay, az = ax, ax
            for e in range(2 * HALO_BLK + 1):
                px, py, pz = p_rows[e]
                vx, vy, vz = v_rows[e][0:1], v_rows[e][1:2], v_rows[e][2:3]
                dx, dy, dz = hx - px, hy - py, hz - pz
                inverse = lax.rsqrt(dx * dx + dy * dy + dz * dz + 1.0)
                inverse_sq = inverse * inverse
                third = inverse_sq * inverse
                along = (dx * vx + dy * vy + dz * vz) * (third * inverse_sq) * 3.0
                ax = ax + (third * vx - along * dx)
                ay = ay + (third * vy - along * dy)
                az = az + (third * vz - along * dz)
            pair_acc[0, at_rows, :] = ax
            pair_acc[1, at_rows, :] = ay
            pair_acc[2, at_rows, :] = az
            return inner

        lax.fori_loop(0, TILE // chunk, strip, 0)
        cols = rows(b, TILE)
        for c in range(3):
            near[c : c + 1, cols] = jnp.sum(pair_acc[c, cols, :].T, axis=0, keepdims=True)
        return carry

    arrival = (2,) + tuple(2 - OFFSETS[k] for k in (2, 3, 0, 1))

    def gather(first, last):
        wide = 256
        band = slice(first * GRID, last * GRID)

        def chunk_of(g, carry):
            cols = rows(g, wide)
            tilt_cols = pl.ds(pl.multiple_of(atoms + g * wide, wide), wide)
            plain = fast_dot(pot3[band, :], zt3[:, cols])
            tilted = fast_dot(pot3[band, :], zt3[:, tilt_cols])
            sa = jnp.zeros((GRID, wide), F32)
            sb, sc = sa, sa
            for slot, p in enumerate(arrival[first:last]):
                here = slice(slot * GRID, (slot + 1) * GRID)
                value = x_spline[p, 0:1, cols]
                sa = sa + x_spline[p, 1:2, cols] * plain[here]
                sb = sb + value * plain[here]
                sc = sc + value * tilted[here]
            for c, part in enumerate((sa * y_t[:, cols], sb * dy_t[:, cols], sc * y_t[:, cols])):
                total = jnp.sum(part, axis=0, keepdims=True)
                far[c : c + 1, cols] = total if first == 0 else far[c : c + 1, cols] + total
            return carry

        lax.fori_loop(0, atoms // wide, chunk_of, 0)

    def put_plane(p, plane):
        hi, lo = split(plane)
        at = arrival.index(p)
        band = slice(at * GRID, (at + 1) * GRID)
        pot3[band, :GRID] = hi
        pot3[band, GRID : 2 * GRID] = lo
        pot3[band, 2 * GRID :] = hi

    def put_vector():
        v = vecs[U]
        for b in range(blocks):
            ext[HALO_BLK + b, 0:3, :] = v[:, b * TILE : (b + 1) * TILE]

    def spread_rim(k):
        rim[k] = spread(OFFSETS[k] + 2, k % 2)

    yz_copy.wait()
    lax.fori_loop(0, blocks, prepare, 0)
    vecs[R] = field[...]
    vecs[U] = field[...] / ip
    for name in (PP, S, X):
        vecs[name] = jnp.zeros((3, atoms), F32)
    scal[...] = jnp.ones_like(scal)
    ra_src[...] = jnp.zeros_like(ra_src)
    put_vector()
    for k in range(len(OFFSETS)):
        spread_rim(k)
    own_plane[...] = spread(2, 0)
    lax.fori_loop(0, blocks, prepare_more, 0)
    prepare_green()
    pl.semaphore_wait(barrier, n - 1)
    for k in range(len(OFFSETS)):
        rim_copy(k).start()
    for c in vec_copies():
        c.start()

    def sweep(it, carry):
        own = own_plane[...]
        for k in range(len(OFFSETS)):
            rim_copy(k).wait_recv()
            own = own + rim_in[k]
        f_src[...] = left_dot(fwd_left, right_dot(own, fwd_right))
        exchange_start(f_src, f_dst, f_ss, f_rs)

        for c in vec_copies():
            c.wait_recv()
        lax.fori_loop(0, blocks, pair_block, 0)

        exchange_all(f_src, f_dst, f_ss, f_rs).wait_recv()
        lines = left_dot(fwd_left, f_dst[...])
        scaled = lines * green[...]
        a_src[...] = left_dot(inv_left, scaled)
        exchange_start(a_src, a_dst, a_ss, a_rs)
        reduce_start(jnp.sum(lines * scaled, axis=0, keepdims=True))
        exchange_all(a_src, a_dst, a_ss, a_rs).wait_recv()
        reduce_middle()
        mine = right_dot(left_dot(inv_left, a_dst[...]), inv_right)
        pot[...] = mine
        for k in (2, 3, 0, 1):
            pot_copy(k).start()
        put_plane(2, mine)
        for c in vec_copies():
            c.wait_send()
        exchange_all(f_src, f_dst, f_ss, f_rs).wait_send()
        exchange_all(a_src, a_dst, a_ss, a_rs).wait_send()
        for k in range(len(OFFSETS)):
            rim_copy(k).wait_send()
        for k in (2, 3):
            pot_copy(k).wait_recv()
            put_plane(2 - OFFSETS[k], pot_in[k])
        gather(0, 3)
        for k in (0, 1):
            pot_copy(k).wait_recv()
            put_plane(2 - OFFSETS[k], pot_in[k])
        gather(3, ORDER)
        u = vecs[U]
        image = ip * u + far[...] - PAIR_C * (near[...] - u)
        gamma, delta = reduce_end()
        beta = jnp.where(it == 0, 0.0, gamma / scal[0, 0:1, 0:1])
        alpha = gamma / (delta - beta * gamma / scal[1, 0:1, 0:1])
        scal[0] = jnp.broadcast_to(gamma, (8, TILE))
        scal[1] = jnp.broadcast_to(alpha, (8, TILE))
        new_p = u + beta * vecs[PP]
        new_s = image + beta * vecs[S]
        vecs[PP] = new_p
        vecs[S] = new_s

        @pl.when(it < ITERS - 1)
        def _():
            residual = vecs[R] - alpha * new_s
            vecs[U] = residual / ip
            for k in range(len(OFFSETS)):
                spread_rim(k)
                rim_copy(k).start()
            put_vector()
            for c in vec_copies():
                c.start()
            own_plane[...] = spread(2, 0)
            vecs[R] = residual
            vecs[X] = vecs[X] + alpha * new_p

        @pl.when(it == ITERS - 1)
        def _():
            dip_a[...] = vecs[X]
            dip_b[...] = new_p
            step_out[...] = jnp.broadcast_to(alpha, (3, atoms))
            res_a[...] = vecs[R]
            res_b[...] = new_s

        for k in range(len(OFFSETS)):
            pot_copy(k).wait_send()
        return carry

    lax.fori_loop(0, ITERS, sweep, 0)


def per_device(n, positions, field, inv_polar, x_spline, yz_spline, tile_list, tile_count):
    atoms = positions.shape[1]
    blocks = atoms // TILE
    nq = NX * NC
    nz = n // nq
    table = basis(GRID)

    def parts(t):
        whole = jnp.asarray(t, F32)
        return split(whole)

    def left_of(t):
        hi, lo = parts(t)
        return jnp.concatenate([hi, lo, hi], axis=1)

    def right_of(t):
        hi, lo = parts(t)
        return jnp.concatenate([hi, hi, lo], axis=0)

    with jax.ensure_compile_time_eval():
        tables = (right_of(table.T), left_of(table), left_of(table.T), right_of(table))
    vm = pl.BlockSpec(memory_space=pltpu.VMEM)
    sm = pl.BlockSpec(memory_space=pltpu.SMEM)
    square = pltpu.VMEM((GRID, GRID), F32)
    sem = pltpu.SemaphoreType.DMA
    out = jax.ShapeDtypeStruct((3, atoms), F32)
    dip_a, dip_b, res_a, res_b, step = pl.pallas_call(
        functools.partial(solve_kernel, n),
        out_shape=(out,) * 5,
        in_specs=[sm, sm] + [vm] * 4 + [pl.BlockSpec(memory_space=pl.ANY)] + [vm] * 4,
        out_specs=(vm,) * 5,
        scratch_shapes=[
            pltpu.VMEM(yz_spline.shape, F32),
            sem,
            pltpu.SMEM((blocks, 2 * HALO_BLK + 1), F32),
            pltpu.VMEM((blocks + 2 * HALO_BLK, 8, TILE), F32),
            pltpu.VMEM((3, atoms, TILE), F32),
            pltpu.VMEM((3, atoms, TILE), F32),
            pltpu.VMEM((3, atoms), F32),
            pltpu.VMEM((3, atoms), F32),
            pltpu.VMEM((GRID, atoms), F32),
            pltpu.VMEM((GRID, atoms), F32),
            pltpu.VMEM((2 * atoms, 2 * GRID), BF16),
            pltpu.VMEM((3 * GRID, 2 * atoms), BF16),
            pltpu.VMEM((2 * GRID, 2 * atoms), BF16),
            pltpu.VMEM((2 * GRID, 2 * atoms), BF16),
            pltpu.VMEM((4, GRID, GRID), F32),
            pltpu.VMEM((4, GRID, GRID), F32),
            square,
            square,
            pltpu.VMEM((4, GRID, GRID), F32),
            pltpu.VMEM((ORDER * GRID, 3 * GRID), BF16),
            square,
            square, square, square, square,
            pltpu.VMEM((8, TILE), F32),
            pltpu.VMEM((nz, 8, TILE), F32),
            pltpu.VMEM((8, TILE), F32),
            pltpu.VMEM((nq, 8, TILE), F32),
            pltpu.VMEM((5, 3, atoms), F32),
            pltpu.VMEM((2, 8, TILE), F32),
            sem((2,)), sem((2,)),
            sem((4,)), sem((4,)),
            sem((4,)), sem((4,)),
            sem, sem, sem, sem,
            sem((nz,)), sem((nz,)),
            sem((nq,)), sem((nq,)),
        ],
        compiler_params=pltpu.CompilerParams(
            collective_id=0, has_side_effects=True, vmem_limit_bytes=56 * 1024 * 1024
        ),
    )(tile_list, tile_count, positions, field, inv_polar.reshape(1, atoms), x_spline.transpose(1, 0, 2), yz_spline,
      *tables)
    return dip_a + step * dip_b, res_a - step * res_b


def solution(mesh):
    both = ("rep", "gx")
    in_specs = (
        P(None, both),
        P(None, both),
        P(both),
        P(None, None, both),
        P(None, both, None),
        P(both, None),
        P(both),
    )
    out_specs = (P(None, both), P(None, both))
    return jax.shard_map(
        functools.partial(per_device, mesh.shape["gx"]),
        mesh=mesh, in_specs=in_specs, out_specs=out_specs, check_vma=False,
    )
```
